256 devices in a mesh: trial: 4 (over x), rows: 8 (over z), cols: 8 (over y, core).
Axes of the slice: x: 4, y: 4, z: 8, core: 2. Of those that a mesh axis runs over, the one named last changes fastest.
Arguments:
- weight_query: bfloat16 [20480, 5120], P(('trial', 'rows'), 'cols'), parts along dimension 0, may hold values from -0.078125 to 0.078125
- low_query: bfloat16 [20480, 32], P(('trial', 'rows')), parts along dimension 0, may hold values from -0.078125 to 0.078125
- high_query: bfloat16 [128, 5120], P('trial', 'cols'), parts along dimension 0, may hold values from -1 to 1
- weight_key: bfloat16 [20480, 1024], P(('trial', 'rows'), 'cols'), parts along dimension 0, may hold values from -0.078125 to 0.078125
- low_key: bfloat16 [20480, 32], P(('trial', 'rows')), parts along dimension 0, may hold values from -0.078125 to 0.078125
- high_key: bfloat16 [128, 1024], P('trial', 'cols'), parts along dimension 0, may hold values from -1 to 1
- weight_value: bfloat16 [20480, 1024], P(('trial', 'rows'), 'cols'), parts along dimension 0, may hold values from -0.078125 to 0.078125
- low_value: bfloat16 [20480, 32], P(('trial', 'rows')), parts along dimension 0, may hold values from -0.078125 to 0.078125
- high_value: bfloat16 [128, 1024], P('trial', 'cols'), parts along dimension 0, may hold values from -1 to 1
- norm_train: float32 [20480], P(('trial', 'rows', 'cols')), parts along dimension 0, may hold values from 0.25 to 1.75
- norm_step: float32 [20480], P(('trial', 'rows', 'cols')), parts along dimension 0, may hold values from -0.3 to 0.3
Outputs:
- serve_query: bfloat16 [20480, 5120], P(('trial', 'cols')), parts along dimension 0
- serve_key: bfloat16 [4096, 5120], P(('trial', 'cols')), parts along dimension 0
- serve_value: bfloat16 [4096, 5120], P(('trial', 'cols')), parts along dimension 0
- serve_norm: bfloat16 [20480], P('trial'), parts along dimension 0
The draws below stay inside these ranges and needn't reach their ends.
There are 4 independent parts, one for each index of `trial`. The reference program is written for one: setup_inputs(seed, part) draws one part's arguments, and reference() takes and returns one part's arrays. A program takes and returns all parts, laid end to end along the dimension named above; each array names one. Nothing has to cross between parts.
All inputs are finite; a program needn't handle non-finite values.
Results may differ from the reference program's by a relative error of at most 0.001.
Values may be sent and summed in bfloat16 or wider, within the bound.
A program may use at most 64 MiB of HBM per device.

```python
import jax
import jax.numpy as jnp

D_MODEL = 5120
Q_DIM = 5120
KV_DIM = 1024
RANK = 32


def levels(own_key, shape, cuts, low, top_value):
    factor_of = 1.0
    for dim, shards_of in cuts:
        steps = jax.random.uniform(jax.random.fold_in(jax.random.fold_in(own_key, 6), dim), (shards_of,), jnp.float32, low / len(cuts), top_value / len(cuts))
        factor_of = factor_of * jnp.repeat(jnp.exp(steps), shape[dim] // shards_of).reshape((-1,) + (1,) * (len(shape) - 1 - dim))
    return factor_of


def gaussian(own_key, dims, width, limit, split=(), dtype=jnp.bfloat16):
    entries = jax.random.normal(own_key, dims, jnp.float32) * width
    if len(split) > 0:
        entries = levels(own_key, dims, split, -0.22, 0.18) * entries
    return jnp.clip(entries, min=-limit, max=limit).astype(dtype)


def setup_inputs(seed: int = 0, part: int = 0) -> dict:
    key_of = jax.random.split(jax.random.key(seed), 12)
    own_keys = jax.random.split(jax.random.fold_in(key_of[11], part), 12)
    return {
        "weight_query": gaussian(own_keys[0], (D_MODEL, Q_DIM), D_MODEL ** -0.5, 0.078125, ((0, 8), (1, 8))),
        "low_query": gaussian(own_keys[1], (D_MODEL, RANK), D_MODEL ** -0.5, 0.078125, ((0, 8),)),
        "high_query": gaussian(own_keys[2], (RANK, Q_DIM), RANK ** -0.5, 1.0, ((1, 8),)),
        "weight_key": gaussian(own_keys[3], (D_MODEL, KV_DIM), D_MODEL ** -0.5, 0.078125, ((0, 8), (1, 8))),
        "low_key": gaussian(own_keys[4], (D_MODEL, RANK), D_MODEL ** -0.5, 0.078125, ((0, 8),)),
        "high_key": gaussian(own_keys[5], (RANK, KV_DIM), RANK ** -0.5, 1.0, ((1, 8),)),
        "weight_value": gaussian(own_keys[6], (D_MODEL, KV_DIM), D_MODEL ** -0.5, 0.078125, ((0, 8), (1, 8))),
        "low_value": gaussian(own_keys[7], (D_MODEL, RANK), D_MODEL ** -0.5, 0.078125, ((0, 8),)),
        "high_value": gaussian(own_keys[8], (RANK, KV_DIM), RANK ** -0.5, 1.0, ((1, 8),)),
        "norm_train": jnp.clip(1.0 + 0.15 * jax.random.normal(own_keys[9], (D_MODEL,), jnp.float32), 0.25, 1.75),
        "norm_step": jnp.clip(jax.random.uniform(own_keys[10], (D_MODEL,), jnp.float32, -0.3, 0.3) * levels(own_keys[10], (D_MODEL,), ((0, 64),), -0.4, 0.0), -0.3, 0.3),
    }


mix_rate = 2.0


def reference(weight_query, low_query, high_query, weight_key, low_key, high_key, weight_value, low_value, high_value, norm_train, norm_step):
    fresh_query = weight_query.astype(jnp.float32) + mix_rate * jnp.dot(low_query, high_query, preferred_element_type=jnp.float32)
    fresh_key = weight_key.astype(jnp.float32) + mix_rate * jnp.dot(low_key, high_key, preferred_element_type=jnp.float32)
    fresh_value = weight_value.astype(jnp.float32) + mix_rate * jnp.dot(low_value, high_value, preferred_element_type=jnp.float32)
    serve_query = fresh_query.T.astype(jnp.bfloat16)
    serve_key = fresh_key.T.astype(jnp.bfloat16)
    serve_value = fresh_value.T.astype(jnp.bfloat16)
    serve_norm = (norm_train + norm_step).astype(jnp.bfloat16)
    return serve_query, serve_key, serve_value, serve_norm
```

```python
import functools

import jax
import jax.numpy as jnp
from jax import lax
from jax.experimental import pallas as pl
from jax.experimental.pallas import tpu as pltpu
from jax.sharding import PartitionSpec as P

MESH = pl.DeviceIdType.MESH
MIX = 2.0
F32 = jnp.float32
BF16 = jnp.bfloat16

N = 8
ROWS = 640
COLS = (640, 128, 128)
WIDTH = sum(COLS)
PIECES = ((0, 128), (128, 128), (256, 128), (384, 64), (448, 64), (512, 128), (640, 128), (768, 128))
NP = len(PIECES)
HALF = NP // 2
RIGHT = [(h, p) for h in range(3) for p in range(NP)] + [(3, p) for p in range(HALF)]
LEFT = [(h, p) for h in range(3) for p in range(NP)] + [(3, p) for p in range(HALF, NP)]
ORDERS = (RIGHT, LEFT)
NS = len(RIGHT)
DEPTH = 4
PAD = 128


def exchange(
    wq, lq, hq, wk, lk, hk, wv, lv, hv, nt, ns,
    buf, gain,
    wq_v, wk_v, wv_v, lq_v, lk_v, lv_v, hq_v, hk_v, hv_v, nt_v, ns_v, gains,
    in_sem, send_sem, recv_sem, gsend, grecv, psend, precv,
):
    z = lax.axis_index("rows")
    c = lax.axis_index("cols")
    right, left = lax.rem(z + 1, N), lax.rem(z + N - 1, N)
    up, down = lax.rem(c + 2, N), lax.rem(c + N - 2, N)
    partner = c + 1 - 2 * lax.rem(c, 2)

    barrier = pltpu.get_barrier_semaphore()
    for who in ({"rows": right}, {"rows": left}, {"cols": up}, {"cols": down}, {"cols": partner}):
        pl.semaphore_signal(barrier, inc=1, device_id=who, device_id_type=MESH)

    loads = []

    def load(src, dst):
        copy = pltpu.make_async_copy(src, dst, in_sem.at[len(loads)])
        copy.start()
        loads.append(copy)
        return copy


    got_lq = load(lq, lq_v)
    got_hq = load(hq, hq_v)
    got_wq = [load(wq.at[:, pl.ds(i * 128, 128)], wq_v.at[i]) for i in range(5)]
    got_nt, got_ns = load(nt, nt_v), load(ns, ns_v)
    got_k = [load(wk, wk_v), load(lk, lk_v), load(hk, hk_v)]
    got_v = [load(wv, wv_v), load(lv, lv_v), load(hv, hv_v)]

    def merged(w, h, lt):
        wt = w.T.astype(F32)
        d = lax.dot_general(h, lt, (((0,), (0,)), ((), ())), preferred_element_type=F32)
        return (wt + MIX * d).astype(BF16)

    def compute(i):
        rows = pl.ds(i * 128, 128)
        if i == 0:
            got_lq.wait()
            got_hq.wait()
        if i < 5:
            got_wq[i].wait()
            buf[z, rows, :] = merged(wq_v[i], hq_v[:, i * 128 : (i + 1) * 128], lq_v[...])
        elif i == 5:
            for x in got_k:
                x.wait()
            buf[z, rows, :] = merged(wk_v[...], hk_v[...], lk_v[...])
        else:
            for x in got_v:
                x.wait()
            buf[z, rows, :] = merged(wv_v[...], hv_v[...], lv_v[...])

    hops = ((right, 1), (left, -1))

    def piece_copy(d, k):
        hop, p = ORDERS[d][k]
        to, sign = hops[d]
        src = lax.rem(z - sign * hop + N, N)
        first, height = PIECES[p]
        ref = buf.at[src, pl.ds(first, height), :]
        return pltpu.make_async_remote_copy(
            src_ref=ref, dst_ref=ref, send_sem=send_sem.at[d, k], recv_sem=recv_sem.at[d, k],
            device_id={"rows": to}, device_id_type=MESH,
        )

    def arrival(d, k):
        hop, p = ORDERS[d][k]
        to, sign = hops[d]
        src = lax.rem(z - sign * (hop + 1) + 2 * N, N)
        first, height = PIECES[p]
        ref = buf.at[src, pl.ds(first, height), :]
        return pltpu.make_async_remote_copy(
            src_ref=ref, dst_ref=ref, send_sem=send_sem.at[d, k], recv_sem=recv_sem.at[d, k],
            device_id={"rows": to}, device_id_type=MESH,
        )

    def gain_copy(d, hop):
        to, sign = hops[d]
        ref = gains.at[c, lax.rem(z - sign * hop + N, N)]
        return pltpu.make_async_remote_copy(
            src_ref=ref, dst_ref=ref, send_sem=gsend.at[d, hop], recv_sem=grecv.at[d, hop],
            device_id={"rows": to}, device_id_type=MESH,
        )

    def gain_arrival(d, hop):
        to, sign = hops[d]
        ref = gains.at[c, lax.rem(z - sign * (hop + 1) + 2 * N, N)]
        return pltpu.make_async_remote_copy(
            src_ref=ref, dst_ref=ref, send_sem=gsend.at[d, hop], recv_sem=grecv.at[d, hop],
            device_id={"rows": to}, device_id_type=MESH,
        )

    pair = c - lax.rem(c, 2)

    def partner_copy(col):
        ref = gains.at[col]
        return pltpu.make_async_remote_copy(
            src_ref=ref, dst_ref=ref, send_sem=psend.at[0], recv_sem=precv.at[0],
            device_id={"cols": partner}, device_id_type=MESH,
        )

    def pair_copy(hop, back):
        ref = gains.at[pl.ds(lax.rem(pair - 2 * (hop + back) + 2 * N, N), 2)]
        return pltpu.make_async_remote_copy(
            src_ref=ref, dst_ref=ref, send_sem=psend.at[1 + hop], recv_sem=precv.at[1 + hop],
            device_id={"cols": up}, device_id_type=MESH,
        )

    def norm_step(k):
        if k == 1:
            for d in range(2):
                gain_copy(d, 0).start()
        elif k in (5, 9, 13):
            hop = (k - 1) // 4
            for d in range(2):
                if hop < 4 - d:
                    gain_arrival(d, hop - 1).wait_recv()
                    gain_copy(d, hop).start()
        elif k == 17:
            gain_arrival(1, 2).wait_recv()
            gain_arrival(0, 3).wait_recv()
            partner_copy(c).start()
        elif k == 19:
            partner_copy(partner).wait_recv()
            pair_copy(0, 0).start()
        elif k in (21, 23):
            hop = (k - 19) // 2
            pair_copy(hop - 1, 1).wait_recv()
            pair_copy(hop, 0).start()
        elif k == 26:
            pair_copy(2, 1).wait_recv()
            lane = lax.broadcasted_iota(jnp.int32, (N, PAD), 1)
            rows = [jnp.zeros((N, PAD), F32) for _ in range(5)]
            for j in range(N):
                v = gains[j].reshape(N, PAD)
                row, off = divmod(80 * j, PAD)
                r = pltpu.roll(v, off, 1) if off else v
                rows[row] = jnp.where((lane >= off) & (lane < off + 80), r, rows[row])
                if off + 80 > PAD:
                    rows[row + 1] = jnp.where(lane < off + 80 - PAD, r, rows[row + 1])
            for j in range(5):
                gain[pl.ds(j, N, stride=5), :] = rows[j]

    compute(0)
    got_nt.wait()
    got_ns.wait()
    gains[c, z, 0:1, 0:80] = (nt_v[...] + ns_v[...]).reshape(1, 80)
    compute(1)
    pl.semaphore_wait(barrier, 5)
    done = 2
    for k in range(NS):
        norm_step(k)
        for d in range(2):
            hop, p = ORDERS[d][k]
            if hop:
                arrival(d, ORDERS[d].index((hop - 1, p))).wait_recv()
            if k >= DEPTH:
                piece_copy(d, k - DEPTH).wait_send()
            piece_copy(d, k).start()
        if k < NP and done < 7:
            compute(done)
            done += 1
    for d in range(2):
        for k in range(NS):
            hop, p = ORDERS[d][k]
            if (hop + 1, p) not in ORDERS[d]:
                arrival(d, k).wait_recv()
    for d in range(2):
        for k in range(NS - DEPTH, NS):
            piece_copy(d, k).wait_send()
        for hop in range(4 - d):
            gain_copy(d, hop).wait_send()
    partner_copy(c).wait_send()
    for hop in range(3):
        pair_copy(hop, 0).wait_send()


def deliver(buf, gain, q, k, v, g, sem):
    copies = []
    for r in range(N):
        at = pl.ds(r * ROWS, ROWS)
        first = 0
        for out, width in zip((q, k, v), COLS):
            copy = pltpu.make_async_copy(buf.at[r, pl.ds(first, width), :], out.at[:, at], sem.at[len(copies)])
            copy.start()
            copies.append(copy)
            first += width
    g[...] = gain[...].astype(BF16)
    for copy in copies:
        copy.wait()


def local(wq, lq, hq, wk, lk, hk, wv, lv, hv, nt, ns):
    hbm = pl.BlockSpec(memory_space=pltpu.HBM)
    vmem = pl.BlockSpec(memory_space=pltpu.VMEM)
    dma = pltpu.SemaphoreType.DMA
    buf, gain = pl.pallas_call(
        exchange,
        name="exchange",
        out_shape=(
            jax.ShapeDtypeStruct((N, WIDTH, ROWS), BF16),
            jax.ShapeDtypeStruct((40, PAD), F32),
        ),
        in_specs=[hbm] * 11,
        out_specs=(vmem, vmem),
        scratch_shapes=[
            pltpu.VMEM((5, ROWS, 128), BF16),
            pltpu.VMEM((ROWS, 128), BF16),
            pltpu.VMEM((ROWS, 128), BF16),
            pltpu.VMEM((32, ROWS), BF16),
            pltpu.VMEM((32, ROWS), BF16),
            pltpu.VMEM((32, ROWS), BF16),
            pltpu.VMEM((32, 640), BF16),
            pltpu.VMEM((32, 128), BF16),
            pltpu.VMEM((32, 128), BF16),
            pltpu.VMEM((80,), F32),
            pltpu.VMEM((80,), F32),
            pltpu.VMEM((N, N, 1, PAD), F32),
            dma((16,)),
            dma((2, NS)),
            dma((2, NS)),
            dma((2, 4)),
            dma((2, 4)),
            dma((4,)),
            dma((4,)),
        ],
        compiler_params=pltpu.CompilerParams(
            collective_id=0, has_side_effects=True, vmem_limit_bytes=24 << 20
        ),
    )(*(pltpu.with_memory_space_constraint(x, pltpu.HBM) for x in (wq, lq.T, hq, wk, lk.T, hk, wv, lv.T, hv, nt, ns)))
    q, k, v, g = pl.pallas_call(
        deliver,
        name="deliver",
        out_shape=(
            jax.ShapeDtypeStruct((COLS[0], N * ROWS), BF16),
            jax.ShapeDtypeStruct((COLS[1], N * ROWS), BF16),
            jax.ShapeDtypeStruct((COLS[2], N * ROWS), BF16),
            jax.ShapeDtypeStruct((40, PAD), BF16),
        ),
        in_specs=[vmem, vmem],
        out_specs=(hbm, hbm, hbm, vmem),
        scratch_shapes=[dma((24,))],
        compiler_params=pltpu.CompilerParams(vmem_limit_bytes=24 << 20),
    )(buf, gain)
    return q, k, v, g.reshape(N * ROWS)


def solution(mesh):
    return jax.shard_map(
        local,
        mesh=mesh,
        in_specs=(
            P(("trial", "rows"), "cols"),
            P(("trial", "rows"), None),
            P("trial", "cols"),
            P(("trial", "rows"), "cols"),
            P(("trial", "rows"), None),
            P("trial", "cols"),
            P(("trial", "rows"), "cols"),
            P(("trial", "rows"), None),
            P("trial", "cols"),
            P(("trial", "rows", "cols")),
            P(("trial", "rows", "cols")),
        ),
        out_specs=(
            P(("trial", "cols"), None),
            P(("trial", "cols"), None),
            P(("trial", "cols"), None),
            P("trial"),
        ),
        check_vma=False,
    )
```

```python
import functools

import jax
import jax.numpy as jnp
from jax import lax
from jax.experimental import pallas as pl
from jax.experimental.pallas import tpu as pltpu
from jax.sharding import PartitionSpec as P

MESH = pl.DeviceIdType.MESH
MIX = 2.0
F32 = jnp.float32
BF16 = jnp.bfloat16

N = 8
ROWS = 640
COLS = (640, 128, 128)
WIDTH = sum(COLS)
PAD = 128
UNIT = 128
PIECES = ((0, 128), (128, 128), (256, 128), (384, 64), (448, 64), (512, 128), (640, 128), (768, 128))
NP = len(PIECES)
UNIT_OF = (0, 1, 2, 3, 3, 4, 5, 6)
ORDERS = tuple(
    [(h, p) for h in range(3) for p in order] + [(3, p) for p in order[: NP // 2]]
    for order in (list(range(NP)), list(range(NP))[::-1])
)
NS = len(ORDERS[0])
DEPTH = 4
FIRST = (24, 20)
assert min(FIRST) >= NS - NP // 2 - NP // 2
SIGN = (1, -1)


def source(z, d, steps):
    return lax.rem(z - SIGN[d] * steps + N, N)


def rows_of(p):
    return pl.ds(*PIECES[p])


def late_slot(d, k):
    return 2 if ORDERS[d][k][0] == 3 else d


def exchange(
    wq, lq, hq, wk, lk, hk, wv, lv, hv, nt, ns,
    buf, gain,
    wq_v, wk_v, wv_v, lq_v, lk_v, lv_v, hq_v, hk_v, hv_v, nt_v, ns_v, gains,
    in_sem, send_sem, recv_sem, gsend, grecv, psend, precv, ready,
):
    z = lax.axis_index("rows")
    c = lax.axis_index("cols")
    to = (lax.rem(z + 1, N), lax.rem(z + N - 1, N))
    up, down = lax.rem(c + 2, N), lax.rem(c + N - 2, N)
    odd = lax.rem(c, 2)
    partner = c + 1 - 2 * odd
    barrier = pltpu.get_barrier_semaphore()

    def signal(sem, **who):
        pl.semaphore_signal(sem, inc=1, device_id=who, device_id_type=MESH)

    pl.when(z < N - 1)(lambda: signal(barrier, rows=to[0]))
    pl.when(z == 0)(lambda: signal(barrier, rows=to[1]))
    pl.when(c < N - 2)(lambda: signal(barrier, cols=up))
    pl.when(c < 2)(lambda: signal(barrier, cols=down))
    pl.when(odd == 1)(lambda: signal(barrier, cols=partner))

    count = [0]

    def load(src, dst):
        copy = pltpu.make_async_copy(src, dst, in_sem.at[count[0]])
        copy.start()
        count[0] += 1
        return copy

    got = {6: [load(lv, lv_v), load(hv, hv_v), load(wv, wv_v)]}
    got[0] = [load(lq, lq_v), load(hq, hq_v), load(wq.at[:, pl.ds(0, UNIT)], wq_v.at[0])]
    got[5] = [load(lk, lk_v), load(hk, hk_v), load(wk, wk_v)]
    for i in (1, 4, 2, 3):
        got[i] = [load(wq.at[:, pl.ds(i * UNIT, UNIT)], wq_v.at[i])]
    got_norm = [load(nt, nt_v), load(ns, ns_v)]

    ahead = [z > 0, z == N - 1, c >= 2, c >= N - 2, odd == 0]
    ahead = sum(x.astype(jnp.int32) for x in ahead)
    pl.when(ahead > 0)(lambda: pl.semaphore_wait(barrier, ahead))
    pl.when(z > 0)(lambda: signal(ready.at[0], rows=to[1]))
    pl.when(z == N - 1)(lambda: signal(ready.at[1], rows=to[0]))
    pl.when(c >= 2)(lambda: signal(ready.at[2], cols=down))
    pl.when(odd == 0)(lambda: signal(ready.at[3], cols=partner))

    def greet(d):
        pl.when(z < N - 1 if d == 0 else z == 0)(lambda: pl.semaphore_wait(ready.at[d], 1))

    def compute(i):
        for x in got[i]:
            x.wait()
        w, h, lt = (
            (wq_v[i], hq_v[:, i * UNIT : (i + 1) * UNIT], lq_v[...]) if i < 5
            else (wk_v[...], hk_v[...], lk_v[...]) if i == 5
            else (wv_v[...], hv_v[...], lv_v[...])
        )
        delta = lax.dot_general(h, lt, (((0,), (0,)), ((), ())), preferred_element_type=F32)
        buf[z, pl.ds(i * UNIT, UNIT), :] = (w.T.astype(F32) + MIX * delta).astype(BF16)

    def piece_copy(d, k, steps_more=0):
        hop, p = ORDERS[d][k]
        ref = buf.at[source(z, d, hop + steps_more), rows_of(p), :]
        return pltpu.make_async_remote_copy(
            src_ref=ref, dst_ref=ref, send_sem=send_sem.at[d, k], recv_sem=recv_sem.at[d, k],
            device_id={"rows": to[d]}, device_id_type=MESH,
        )

    def arrived(d, k):
        piece_copy(d, k, 1).wait_recv()

    def gain_copy(d, hop, steps_more=0):
        ref = gains.at[c, source(z, d, hop + steps_more)]
        return pltpu.make_async_remote_copy(
            src_ref=ref, dst_ref=ref, send_sem=gsend.at[d, hop], recv_sem=grecv.at[d, hop],
            device_id={"rows": to[d]}, device_id_type=MESH,
        )

    def partner_copy(col):
        ref = gains.at[col]
        return pltpu.make_async_remote_copy(
            src_ref=ref, dst_ref=ref, send_sem=psend.at[0], recv_sem=precv.at[0],
            device_id={"cols": partner}, device_id_type=MESH,
        )

    def pair_copy(hop, steps_more=0):
        ref = gains.at[pl.ds(lax.rem(c - odd - 2 * (hop + steps_more) + N, N), 2)]
        return pltpu.make_async_remote_copy(
            src_ref=ref, dst_ref=ref, send_sem=psend.at[1 + hop], recv_sem=precv.at[1 + hop],
            device_id={"cols": up}, device_id_type=MESH,
        )

    def norm_step(k):
        if k in (4, 7, 10, 13):
            hop = (k - 4) // 3
            for d in range(2):
                if hop < 4 - d:
                    if hop:
                        gain_copy(d, hop - 1, 1).wait_recv()
                    gain_copy(d, hop).start()
        elif k == 16:
            gain_copy(1, 2, 1).wait_recv()
            gain_copy(0, 3, 1).wait_recv()
            pl.when(odd == 1)(lambda: pl.semaphore_wait(ready.at[3], 1))
            partner_copy(c).start()
        elif k == 17:
            partner_copy(partner).wait_recv()
            pl.when(c < N - 2)(lambda: pl.semaphore_wait(ready.at[2], 1))
            pair_copy(0).start()
        elif k in (18, 19):
            pair_copy(k - 18, 1).wait_recv()
            pair_copy(k - 17).start()

    def norm_end():
        pair_copy(2, 1).wait_recv()
        lane = lax.broadcasted_iota(jnp.int32, (N, PAD), 1)
        rows = [jnp.zeros((N, PAD), F32) for _ in range(5)]
        for j in range(N):
            row, off = divmod(80 * j, PAD)
            v = gains[j].reshape(N, PAD)
            v = pltpu.roll(v, off, 1) if off else v
            rows[row] = jnp.where((lane >= off) & (lane < off + 80), v, rows[row])
            if off + 80 > PAD:
                rows[row + 1] = jnp.where(lane < off + 80 - PAD, v, rows[row + 1])
        for j in range(5):
            gain[pl.ds(j, N, stride=5), :] = rows[j]
        for d in range(2):
            for hop in range(4 - d):
                gain_copy(d, hop).wait_send()
        partner_copy(c).wait_send()
        for hop in range(3):
            pair_copy(hop).wait_send()

    units = (6, 0, 5, 1, 4, 2, 3)

    @pl.when(z == 0)
    def _():
        for i in units:
            compute(i)
        for d in range(2):
            greet(d)
            for k in range(DEPTH):
                piece_copy(d, k).start()

    @pl.when(z > 0)
    def _():
        done = 2
        for i in units[:done]:
            compute(i)
        for k in range(DEPTH):
            for d in (1, 0):
                if k == 0:
                    greet(d)
                piece_copy(d, k).start()
                if done < len(units):
                    compute(units[done])
                    done += 1

    for x in got_norm:
        x.wait()
    gains[c, z, 0:1, 0:80] = (nt_v[...] + ns_v[...]).reshape(1, 80)

    def item(k):
        for d in (1, 0):
            hop, p = ORDERS[d][k]
            if hop:
                arrived(d, k - NP)
            piece_copy(d, k - DEPTH).wait_send()
            piece_copy(d, k).start()

    def drain(last):
        for d in range(2):
            for k in range(last - DEPTH, last):
                piece_copy(d, k).wait_send()
            for k in range(last - NP, last):
                arrived(d, k)

    low, high = sorted(FIRST)
    for k in range(DEPTH, low):
        norm_step(k)
        item(k)
    norm_end()
    for parity in range(2):

        @pl.when(odd == parity)
        def _():
            for k in range(low, FIRST[parity]):
                item(k)
            drain(FIRST[parity])


def finish(buf, late, send_sem, recv_sem):
    z = lax.axis_index("rows")
    odd = lax.rem(lax.axis_index("cols"), 2)
    to = (lax.rem(z + 1, N), lax.rem(z + N - 1, N))
    barrier = pltpu.get_barrier_semaphore()
    for d in range(2):
        pl.semaphore_signal(barrier, inc=1, device_id={"rows": to[d]}, device_id_type=MESH)
    pl.semaphore_wait(barrier, 2)

    def piece_copy(d, k):
        hop, p = ORDERS[d][k]
        return pltpu.make_async_remote_copy(
            src_ref=buf.at[source(z, d, hop), rows_of(p), :], dst_ref=late.at[late_slot(d, k), rows_of(p), :],
            send_sem=send_sem.at[d, k], recv_sem=recv_sem.at[d, k],
            device_id={"rows": to[d]}, device_id_type=MESH,
        )

    def send(k):
        for d in (1, 0):
            piece_copy(d, k).start()

    def wait(k):
        for d in (1, 0):
            piece_copy(d, k).wait()

    low, high = sorted(FIRST)
    pl.when(odd == FIRST.index(low))(lambda: [send(k) for k in range(low, high)] and None)
    for k in range(high, NS):
        send(k)
    pl.when(odd == FIRST.index(low))(lambda: [wait(k) for k in range(low, high)] and None)
    for k in range(high, NS):
        wait(k)


def spans(pieces):
    runs = []
    for p in sorted(pieces):
        first, height = PIECES[p]
        if runs and runs[-1][1] == first and first not in (640, 768):
            runs[-1][1] = first + height
        else:
            runs.append([first, first + height])
    return runs


def write_out(outs, z, sem, jobs):
    copies = []
    for block, distance, pieces in jobs:
        at = pl.ds(pl.multiple_of(lax.rem(z + distance + N, N) * ROWS, ROWS), ROWS)
        for first, last in spans(pieces):
            which = 0 if first < 640 else 1 if first < 768 else 2
            copies.append(
                pltpu.make_async_copy(
                    block.at[pl.ds(first, last - first), :],
                    outs[which].at[pl.ds(first - sum(COLS[:which]), last - first), at],
                    sem.at[len(copies)],
                )
            )
    for copy in copies:
        copy.start()
    for copy in copies:
        copy.wait()


def arrivals(ks):
    blocks = {}
    for d in range(2):
        for k in ks:
            hop, p = ORDERS[d][k]
            distance = -SIGN[d] * (hop + 1)
            blocks.setdefault(4 if distance == -4 else distance, []).append(p)
    return blocks


def deliver(buf, gain, q, k, v, g, sem):
    z = lax.axis_index("rows")
    odd = lax.rem(lax.axis_index("cols"), 2)
    g[...] = gain[...].astype(BF16)
    for parity in range(2):

        @pl.when(odd == parity)
        def _():
            blocks = {0: list(range(NP))} | arrivals(range(FIRST[parity]))
            write_out((q, k, v), z, sem, [(buf.at[lax.rem(z + b + N, N)], b, ps) for b, ps in blocks.items()])


def deliver_late(late, q_in, k_in, v_in, q, k, v, sem):
    z = lax.axis_index("rows")
    odd = lax.rem(lax.axis_index("cols"), 2)
    slots = {-3: 0, 3: 1, 4: 2}
    for parity in range(2):

        @pl.when(odd == parity)
        def _():
            blocks = arrivals(range(FIRST[parity], NS))
            write_out((q, k, v), z, sem, [(late.at[slots[b]], b, ps) for b, ps in blocks.items()])


def local(wq, lq, hq, wk, lk, hk, wv, lv, hv, nt, ns):
    hbm = pl.BlockSpec(memory_space=pltpu.HBM)
    vmem = pl.BlockSpec(memory_space=pltpu.VMEM)
    dma = pltpu.SemaphoreType.DMA
    limit = 16 << 20
    args = (wq, lq.T, hq, wk, lk.T, hk, wv, lv.T, hv, nt, ns)
    buf, gain = pl.pallas_call(
        exchange,
        name="exchange",
        out_shape=(
            jax.ShapeDtypeStruct((N, WIDTH, ROWS), BF16),
            jax.ShapeDtypeStruct((40, PAD), F32),
        ),
        in_specs=[hbm] * 11,
        out_specs=(vmem, vmem),
        scratch_shapes=[
            pltpu.VMEM((5, ROWS, UNIT), BF16),
            pltpu.VMEM((ROWS, UNIT), BF16),
            pltpu.VMEM((ROWS, UNIT), BF16),
            pltpu.VMEM((32, ROWS), BF16),
            pltpu.VMEM((32, ROWS), BF16),
            pltpu.VMEM((32, ROWS), BF16),
            pltpu.VMEM((32, COLS[0]), BF16),
            pltpu.VMEM((32, COLS[1]), BF16),
            pltpu.VMEM((32, COLS[2]), BF16),
            pltpu.VMEM((80,), F32),
            pltpu.VMEM((80,), F32),
            pltpu.VMEM((N, N, 1, PAD), F32),
            dma((16,)),
            dma((2, NS)),
            dma((2, NS)),
            dma((2, 4)),
            dma((2, 4)),
            dma((4,)),
            dma((4,)),
            pltpu.SemaphoreType.REGULAR((4,)),
        ],
        compiler_params=pltpu.CompilerParams(collective_id=0, has_side_effects=True, vmem_limit_bytes=limit),
    )(*(pltpu.with_memory_space_constraint(x, pltpu.HBM) for x in args))
    wide = [jax.ShapeDtypeStruct((width, N * ROWS), BF16) for width in COLS]
    q, k, v, g = pl.pallas_call(
        deliver,
        name="deliver",
        out_shape=(*wide, jax.ShapeDtypeStruct((40, PAD), BF16)),
        in_specs=[vmem, vmem],
        out_specs=(hbm, hbm, hbm, vmem),
        scratch_shapes=[dma((32,))],
        compiler_params=pltpu.CompilerParams(vmem_limit_bytes=limit, has_side_effects=True),
    )(buf, gain)
    late = pl.pallas_call(
        finish,
        name="finish",
        out_shape=jax.ShapeDtypeStruct((3, WIDTH, ROWS), BF16),
        in_specs=[vmem],
        out_specs=vmem,
        scratch_shapes=[dma((2, NS)), dma((2, NS))],
        compiler_params=pltpu.CompilerParams(collective_id=1, has_side_effects=True, vmem_limit_bytes=limit),
    )(buf)
    q, k, v = pl.pallas_call(
        deliver_late,
        name="deliver_late",
        out_shape=tuple(wide),
        in_specs=[vmem, hbm, hbm, hbm],
        out_specs=(hbm, hbm, hbm),
        scratch_shapes=[dma((16,))],
        input_output_aliases={1: 0, 2: 1, 3: 2},
        compiler_params=pltpu.CompilerParams(vmem_limit_bytes=limit),
    )(late, q, k, v)
    return q, k, v, g.reshape(N * ROWS)


def solution(mesh):
    return jax.shard_map(
        local,
        mesh=mesh,
        in_specs=(
            P(("trial", "rows"), "cols"),
            P(("trial", "rows"), None),
            P("trial", "cols"),
            P(("trial", "rows"), "cols"),
            P(("trial", "rows"), None),
            P("trial", "cols"),
            P(("trial", "rows"), "cols"),
            P(("trial", "rows"), None),
            P("trial", "cols"),
            P(("trial", "rows", "cols")),
            P(("trial", "rows", "cols")),
        ),
        out_specs=(
            P(("trial", "cols"), None),
            P(("trial", "cols"), None),
            P(("trial", "cols"), None),
            P("trial"),
        ),
        check_vma=False,
    )
```

```python
import functools

import jax
import jax.numpy as jnp
from jax import lax
from jax.experimental import pallas as pl
from jax.experimental.pallas import tpu as pltpu
from jax.sharding import PartitionSpec as P

MESH = pl.DeviceIdType.MESH
MIX = 2.0
F32 = jnp.float32
BF16 = jnp.bfloat16

N = 8
ROWS = 640
COLS = (640, 128, 128)
WIDTH = sum(COLS)
PAD = 128
UNIT = 128
HOPS = (
    ((0, 128), (128, 320), (448, 320), (768, 128)),
    ((0, 128), (128, 320), (448, 448)),
    ((0, 448), (448, 448)),
    ((0, 384), (384, 64)),
)
RIGHT = [(h, *piece) for h, pieces in enumerate(HOPS) for piece in pieces]
LEFT = [(h, WIDTH - first - height, height) for h, first, height in RIGHT[:-2]] + [(3, 448, 448), (3, 384, 64)]
ORDERS = (RIGHT, LEFT)
NS = len(RIGHT)
LAST = NS - 1
DEPTH = 2
FIRST = (9, 7)
SIGN = (1, -1)


def source(z, d, steps):
    return lax.rem(z - SIGN[d] * steps + N, N)


def rows_of(d, k):
    return pl.ds(*ORDERS[d][k][1:])


def needs(d, k):
    hop, first, height = ORDERS[d][k]
    return [
        i for i, (h, f, n) in enumerate(ORDERS[d])
        if h == hop - 1 and f < first + height and first < f + n
    ]


def if_sent(z, d, k, act):
    if k < LAST:
        act()
    else:
        pl.when(z < N - 1 if d == 0 else z == 1)(act)


def if_received(z, d, k, act):
    if k < LAST:
        act()
    else:
        pl.when(z > 0 if d == 0 else z == 0)(act)


def exchange(
    wq, lq, hq, wk, lk, hk, wv, lv, hv, nt, ns,
    buf, gain,
    wq_v, wk_v, wv_v, lq_v, lk_v, lv_v, hq_v, hk_v, hv_v, nt_v, ns_v, gains,
    in_sem, send_sem, recv_sem, gsend, grecv, psend, precv, ready,
):
    z = lax.axis_index("rows")
    c = lax.axis_index("cols")
    to = (lax.rem(z + 1, N), lax.rem(z + N - 1, N))
    up, down = lax.rem(c + 2, N), lax.rem(c + N - 2, N)
    odd = lax.rem(c, 2)
    partner = c + 1 - 2 * odd
    barrier = pltpu.get_barrier_semaphore()

    def signal(sem, **who):
        pl.semaphore_signal(sem, inc=1, device_id=who, device_id_type=MESH)

    pl.when(z < N - 1)(lambda: signal(barrier, rows=to[0]))
    pl.when(z == 0)(lambda: signal(barrier, rows=to[1]))
    pl.when(c < N - 2)(lambda: signal(barrier, cols=up))
    pl.when(c < 2)(lambda: signal(barrier, cols=down))
    pl.when(odd == 1)(lambda: signal(barrier, cols=partner))

    count = [0]

    def load(src, dst):
        copy = pltpu.make_async_copy(src, dst, in_sem.at[count[0]])
        copy.start()
        count[0] += 1
        return copy

    got = {6: [load(lv, lv_v), load(hv, hv_v), load(wv, wv_v)]}
    got[0] = [load(lq, lq_v), load(hq, hq_v), load(wq.at[:, pl.ds(0, UNIT)], wq_v.at[0])]
    got[5] = [load(lk, lk_v), load(hk, hk_v), load(wk, wk_v)]
    for i in (1, 4, 2, 3):
        got[i] = [load(wq.at[:, pl.ds(i * UNIT, UNIT)], wq_v.at[i])]
    got_norm = [load(nt, nt_v), load(ns, ns_v)]

    ahead = [z > 0, z == N - 1, c >= 2, c >= N - 2, odd == 0]
    ahead = sum(x.astype(jnp.int32) for x in ahead)
    pl.when(ahead > 0)(lambda: pl.semaphore_wait(barrier, ahead))
    pl.when(z > 0)(lambda: signal(ready.at[0], rows=to[1]))
    pl.when(z == N - 1)(lambda: signal(ready.at[1], rows=to[0]))
    pl.when(c >= 2)(lambda: signal(ready.at[2], cols=down))
    pl.when(odd == 0)(lambda: signal(ready.at[3], cols=partner))

    def greet(d):
        pl.when(z < N - 1 if d == 0 else z == 0)(lambda: pl.semaphore_wait(ready.at[d], 1))

    def compute(i):
        for x in got[i]:
            x.wait()
        w, h, lt = (
            (wq_v[i], hq_v[:, i * UNIT : (i + 1) * UNIT], lq_v[...]) if i < 5
            else (wk_v[...], hk_v[...], lk_v[...]) if i == 5
            else (wv_v[...], hv_v[...], lv_v[...])
        )
        delta = lax.dot_general(h, lt, (((0,), (0,)), ((), ())), preferred_element_type=F32)
        buf[z, pl.ds(i * UNIT, UNIT), :] = (w.T.astype(F32) + MIX * delta).astype(BF16)

    def piece_copy(d, k, steps_more=0):
        ref = buf.at[source(z, d, ORDERS[d][k][0] + steps_more), rows_of(d, k), :]
        return pltpu.make_async_remote_copy(
            src_ref=ref, dst_ref=ref, send_sem=send_sem.at[d, k], recv_sem=recv_sem.at[d, k],
            device_id={"rows": to[d]}, device_id_type=MESH,
        )

    def gain_copy(d, hop, steps_more=0):
        ref = gains.at[c, source(z, d, hop + steps_more)]
        return pltpu.make_async_remote_copy(
            src_ref=ref, dst_ref=ref, send_sem=gsend.at[d, hop], recv_sem=grecv.at[d, hop],
            device_id={"rows": to[d]}, device_id_type=MESH,
        )

    def partner_copy(col):
        ref = gains.at[col]
        return pltpu.make_async_remote_copy(
            src_ref=ref, dst_ref=ref, send_sem=psend.at[0], recv_sem=precv.at[0],
            device_id={"cols": partner}, device_id_type=MESH,
        )

    def pair_copy(hop, steps_more=0):
        ref = gains.at[pl.ds(lax.rem(c - odd - 2 * (hop + steps_more) + N, N), 2)]
        return pltpu.make_async_remote_copy(
            src_ref=ref, dst_ref=ref, send_sem=psend.at[1 + hop], recv_sem=precv.at[1 + hop],
            device_id={"cols": up}, device_id_type=MESH,
        )

    def norm_step(k):
        hop = {2: 1, 3: 2, 5: 3}.get(k)
        for d in range(2):
            if hop is not None and hop < 4 - d:
                gain_copy(d, hop - 1, 1).wait_recv()
                gain_copy(d, hop).start()

    def norm_end():
        gain_copy(1, 2, 1).wait_recv()
        gain_copy(0, 3, 1).wait_recv()
        pl.when(odd == 1)(lambda: pl.semaphore_wait(ready.at[3], 1))
        partner_copy(c).start()
        partner_copy(partner).wait_recv()
        pl.when(c < N - 2)(lambda: pl.semaphore_wait(ready.at[2], 1))
        for hop in range(3):
            pair_copy(hop).start()
            pair_copy(hop, 1).wait_recv()
        lane = lax.broadcasted_iota(jnp.int32, (N, PAD), 1)
        rows = [jnp.zeros((N, PAD), F32) for _ in range(5)]
        for j in range(N):
            row, off = divmod(80 * j, PAD)
            v = gains[j].reshape(N, PAD)
            v = pltpu.roll(v, off, 1) if off else v
            rows[row] = jnp.where((lane >= off) & (lane < off + 80), v, rows[row])
            if off + 80 > PAD:
                rows[row + 1] = jnp.where(lane < off + 80 - PAD, v, rows[row + 1])
        for j in range(5):
            gain[pl.ds(j, N, stride=5), :] = rows[j]
        for d in range(2):
            for hop in range(4 - d):
                gain_copy(d, hop).wait_send()
        partner_copy(c).wait_send()
        for hop in range(3):
            pair_copy(hop).wait_send()

    def begin(d):
        greet(d)
        gain_copy(d, 0).start()
        piece_copy(d, 0).start()

    for x in got_norm:
        x.wait()
    gains[c, z, 0:1, 0:80] = (nt_v[...] + ns_v[...]).reshape(1, 80)

    @pl.when(z == 0)
    def _():
        for i in (0, 6, 1, 2, 3, 4, 5):
            compute(i)
        for d in range(2):
            begin(d)
            piece_copy(d, 1).start()

    @pl.when(z > 0)
    def _():
        for i in (6, 0, 5):
            compute(i)
        begin(1)
        compute(1)
        begin(0)
        for i in (4, 2, 3):
            compute(i)
        for d in (1, 0):
            piece_copy(d, 1).start()

    def item(k, met):
        for d in (1, 0):
            for i in needs(d, k):
                if (d, i) not in met:
                    piece_copy(d, i, 1).wait_recv()
                    met.add((d, i))
            piece_copy(d, k - DEPTH).wait_send()
            piece_copy(d, k).start()

    def drain(last, met):
        for d in range(2):
            for k in range(last - DEPTH, last):
                piece_copy(d, k).wait_send()
            for k in range(last):
                if (d, k) not in met:
                    piece_copy(d, k, 1).wait_recv()

    met = set()
    low = min(FIRST)
    for k in range(DEPTH, low):
        norm_step(k)
        item(k, met)
    norm_end()
    for parity in range(2):

        @pl.when(odd == parity)
        def _():
            mine = set(met)
            for k in range(low, FIRST[parity]):
                item(k, mine)
            drain(FIRST[parity], mine)


def finish(buf, late, send_sem, recv_sem):
    z = lax.axis_index("rows")
    odd = lax.rem(lax.axis_index("cols"), 2)
    to = (lax.rem(z + 1, N), lax.rem(z + N - 1, N))
    barrier = pltpu.get_barrier_semaphore()
    for d in range(2):
        pl.semaphore_signal(barrier, inc=1, device_id={"rows": to[d]}, device_id_type=MESH)
    pl.semaphore_wait(barrier, 2)

    def piece_copy(d, k, first):
        hop = ORDERS[d][k][0]
        here = late.at[d] if needs(d, k)[0] >= first else buf.at[source(z, d, hop)]
        return pltpu.make_async_remote_copy(
            src_ref=here.at[rows_of(d, k), :], dst_ref=late.at[2 if hop == 3 else d, rows_of(d, k), :],
            send_sem=send_sem.at[d, k], recv_sem=recv_sem.at[d, k],
            device_id={"rows": to[d]}, device_id_type=MESH,
        )

    for parity, first in enumerate(FIRST):

        @pl.when(odd == parity)
        def _():
            met = set()
            for k in range(first, NS):
                for d in (1, 0):
                    for i in needs(d, k):
                        if i >= first and (d, i) not in met:
                            piece_copy(d, i, first).wait_recv()
                            met.add((d, i))
                    if_sent(z, d, k, lambda d=d, k=k: piece_copy(d, k, first).start())
            for k in range(first, NS):
                for d in (1, 0):
                    if_sent(z, d, k, lambda d=d, k=k: piece_copy(d, k, first).wait_send())
                    if (d, k) not in met:
                        if_received(z, d, k, lambda d=d, k=k: piece_copy(d, k, first).wait_recv())


def write_out(outs, z, sem, blocks):
    copies = []
    for block, distance in blocks:
        at = pl.ds(pl.multiple_of(lax.rem(z + distance + N, N) * ROWS, ROWS), ROWS)
        first = 0
        for out, width in zip(outs, COLS):
            copies.append(pltpu.make_async_copy(block.at[pl.ds(first, width), :], out.at[:, at], sem.at[len(copies)]))
            first += width
    for copy in copies:
        copy.start()
    for copy in copies:
        copy.wait()


def early(parity):
    return (0, 1, -1, 2, -2) if FIRST[parity] == 7 else (0, 1, -1, 2, -2, 3, -3)


def deliver(buf, gain, q, k, v, g, sem):
    z = lax.axis_index("rows")
    odd = lax.rem(lax.axis_index("cols"), 2)
    g[...] = gain[...].astype(BF16)
    for parity in range(2):

        @pl.when(odd == parity)
        def _():
            write_out((q, k, v), z, sem, [(buf.at[lax.rem(z + b + N, N)], b) for b in early(parity)])


def deliver_late(late, q_in, k_in, v_in, q, k, v, sem):
    z = lax.axis_index("rows")
    odd = lax.rem(lax.axis_index("cols"), 2)
    for parity in range(2):

        @pl.when(odd == parity)
        def _():
            blocks = [(late.at[slot], b) for slot, b in enumerate((-3, 3, 4)) if b not in early(parity)]
            write_out((q, k, v), z, sem, blocks)


def local(wq, lq, hq, wk, lk, hk, wv, lv, hv, nt, ns):
    hbm = pl.BlockSpec(memory_space=pltpu.HBM)
    vmem = pl.BlockSpec(memory_space=pltpu.VMEM)
    dma = pltpu.SemaphoreType.DMA
    limit = 16 << 20
    args = (wq, lq.T, hq, wk, lk.T, hk, wv, lv.T, hv, nt, ns)
    buf, gain = pl.pallas_call(
        exchange,
        name="exchange",
        out_shape=(
            jax.ShapeDtypeStruct((N, WIDTH, ROWS), BF16),
            jax.ShapeDtypeStruct((40, PAD), F32),
        ),
        in_specs=[hbm] * 11,
        out_specs=(vmem, vmem),
        scratch_shapes=[
            pltpu.VMEM((5, ROWS, UNIT), BF16),
            pltpu.VMEM((ROWS, UNIT), BF16),
            pltpu.VMEM((ROWS, UNIT), BF16),
            pltpu.VMEM((32, ROWS), BF16),
            pltpu.VMEM((32, ROWS), BF16),
            pltpu.VMEM((32, ROWS), BF16),
            pltpu.VMEM((32, COLS[0]), BF16),
            pltpu.VMEM((32, COLS[1]), BF16),
            pltpu.VMEM((32, COLS[2]), BF16),
            pltpu.VMEM((80,), F32),
            pltpu.VMEM((80,), F32),
            pltpu.VMEM((N, N, 1, PAD), F32),
            dma((16,)),
            dma((2, NS)),
            dma((2, NS)),
            dma((2, 4)),
            dma((2, 4)),
            dma((4,)),
            dma((4,)),
            pltpu.SemaphoreType.REGULAR((4,)),
        ],
        compiler_params=pltpu.CompilerParams(collective_id=0, has_side_effects=True, vmem_limit_bytes=limit),
    )(*(pltpu.with_memory_space_constraint(x, pltpu.HBM) for x in args))
    wide = [jax.ShapeDtypeStruct((width, N * ROWS), BF16) for width in COLS]
    q, k, v, g = pl.pallas_call(
        deliver,
        name="deliver",
        out_shape=(*wide, jax.ShapeDtypeStruct((40, PAD), BF16)),
        in_specs=[vmem, vmem],
        out_specs=(hbm, hbm, hbm, vmem),
        scratch_shapes=[dma((32,))],
        compiler_params=pltpu.CompilerParams(vmem_limit_bytes=limit, has_side_effects=True),
    )(buf, gain)
    late = pl.pallas_call(
        finish,
        name="finish",
        out_shape=jax.ShapeDtypeStruct((3, WIDTH, ROWS), BF16),
        in_specs=[vmem],
        out_specs=vmem,
        scratch_shapes=[dma((2, NS)), dma((2, NS))],
        compiler_params=pltpu.CompilerParams(collective_id=1, has_side_effects=True, vmem_limit_bytes=limit),
    )(buf)
    q, k, v = pl.pallas_call(
        deliver_late,
        name="deliver_late",
        out_shape=tuple(wide),
        in_specs=[vmem, hbm, hbm, hbm],
        out_specs=(hbm, hbm, hbm),
        scratch_shapes=[dma((16,))],
        input_output_aliases={1: 0, 2: 1, 3: 2},
        compiler_params=pltpu.CompilerParams(vmem_limit_bytes=limit),
    )(late, q, k, v)
    return q, k, v, g.reshape(N * ROWS)


def solution(mesh):
    return jax.shard_map(
        local,
        mesh=mesh,
        in_specs=(
            P(("trial", "rows"), "cols"),
            P(("trial", "rows"), None),
            P("trial", "cols"),
            P(("trial", "rows"), "cols"),
            P(("trial", "rows"), None),
            P("trial", "cols"),
            P(("trial", "rows"), "cols"),
            P(("trial", "rows"), None),
            P("trial", "cols"),
            P(("trial", "rows", "cols")),
            P(("trial", "rows", "cols")),
        ),
        out_specs=(
            P(("trial", "cols"), None),
            P(("trial", "cols"), None),
            P(("trial", "cols"), None),
            P("trial"),
        ),
        check_vma=False,
    )
```

```python
import functools

import jax
import jax.numpy as jnp
from jax import lax
from jax.experimental import pallas as pl
from jax.experimental.pallas import tpu as pltpu
from jax.sharding import PartitionSpec as P

MESH = pl.DeviceIdType.MESH
MIX = 2.0
F32 = jnp.float32
BF16 = jnp.bfloat16

N = 8
ROWS = 640
COLS = (640, 128, 128)
WIDTH = sum(COLS)
PAD = 128
UNIT = 128
HOPS = (
    ((0, 128), (128, 320), (448, 320), (768, 128)),
    ((0, 128), (128, 320), (448, 448)),
    ((0, 448), (448, 448)),
    ((0, 368), (368, 80)),
)
RIGHT = [(h, *piece) for h, pieces in enumerate(HOPS) for piece in pieces]
LEFT = [(h, WIDTH - first - height, height) for h, first, height in RIGHT[:-2]] + [(3, 448, 448), (3, 368, 80)]
ORDERS = (RIGHT, LEFT)
NS = len(RIGHT)
LAST = NS - 1
DEPTH = 2
FIRST = (9, 7)
SIGN = (1, -1)


def source(z, d, steps):
    return lax.rem(z - SIGN[d] * steps + N, N)


def rows_of(d, k):
    return pl.ds(*ORDERS[d][k][1:])


def needs(d, k):
    hop, first, height = ORDERS[d][k]
    return [
        i for i, (h, f, n) in enumerate(ORDERS[d])
        if h == hop - 1 and f < first + height and first < f + n
    ]


def if_sent(z, d, k, act):
    if k < LAST:
        act()
    else:
        pl.when(z < N - 1 if d == 0 else z == 1)(act)


def if_received(z, d, k, act):
    if k < LAST:
        act()
    else:
        pl.when(z > 0 if d == 0 else z == 0)(act)


def exchange(
    wq, lq, hq, wk, lk, hk, wv, lv, hv, nt, ns,
    buf, gain,
    wq_v, wk_v, wv_v, lq_v, lk_v, lv_v, hq_v, hk_v, hv_v, nt_v, ns_v, gains,
    in_sem, send_sem, recv_sem, gsend, grecv, psend, precv, ready,
):
    z = lax.axis_index("rows")
    c = lax.axis_index("cols")
    to = (lax.rem(z + 1, N), lax.rem(z + N - 1, N))
    up, down = lax.rem(c + 2, N), lax.rem(c + N - 2, N)
    odd = lax.rem(c, 2)
    partner = c + 1 - 2 * odd
    barrier = pltpu.get_barrier_semaphore()

    def signal(sem, **who):
        pl.semaphore_signal(sem, inc=1, device_id=who, device_id_type=MESH)

    pl.when(z < N - 1)(lambda: signal(barrier, rows=to[0]))
    pl.when(z == 0)(lambda: signal(barrier, rows=to[1]))
    pl.when(c < N - 2)(lambda: signal(barrier, cols=up))
    pl.when(c < 2)(lambda: signal(barrier, cols=down))
    pl.when(odd == 1)(lambda: signal(barrier, cols=partner))

    count = [0]

    def load(src, dst):
        copy = pltpu.make_async_copy(src, dst, in_sem.at[count[0]])
        copy.start()
        count[0] += 1
        return copy

    got = {6: [load(lv, lv_v), load(hv, hv_v), load(wv, wv_v)]}
    got[0] = [load(lq, lq_v), load(hq, hq_v), load(wq.at[:, pl.ds(0, UNIT)], wq_v.at[0])]
    got_norm = [load(nt, nt_v), load(ns, ns_v)]
    got[5] = [load(lk, lk_v), load(hk, hk_v), load(wk, wk_v)]
    for i in (1, 4, 2, 3):
        got[i] = [load(wq.at[:, pl.ds(i * UNIT, UNIT)], wq_v.at[i])]

    def greet(d):
        pl.when(z < N - 1 if d == 0 else z == 0)(lambda: pl.semaphore_wait(ready.at[d], 1))

    def compute(i):
        for x in got[i]:
            x.wait()
        w, h, lt = (
            (wq_v[i], hq_v[:, i * UNIT : (i + 1) * UNIT], lq_v[...]) if i < 5
            else (wk_v[...], hk_v[...], lk_v[...]) if i == 5
            else (wv_v[...], hv_v[...], lv_v[...])
        )
        delta = lax.dot_general(h, lt, (((0,), (0,)), ((), ())), preferred_element_type=F32)
        buf[z, pl.ds(i * UNIT, UNIT), :] = (w.T.astype(F32) + MIX * delta).astype(BF16)

    rightmost = (z == 0) | (z == N - 1)

    @pl.when(rightmost)
    def _():
        compute(0)
        compute(6)

    @pl.when(jnp.logical_not(rightmost))
    def _():
        compute(6)
        compute(0)

    ahead = [z > 0, z == N - 1, c >= 2, c >= N - 2, odd == 0]
    ahead = sum(x.astype(jnp.int32) for x in ahead)
    pl.when(ahead > 0)(lambda: pl.semaphore_wait(barrier, ahead))
    pl.when(z > 0)(lambda: signal(ready.at[0], rows=to[1]))
    pl.when(z == N - 1)(lambda: signal(ready.at[1], rows=to[0]))
    pl.when(c >= 2)(lambda: signal(ready.at[2], cols=down))
    pl.when(odd == 0)(lambda: signal(ready.at[3], cols=partner))

    def piece_copy(d, k, steps_more=0):
        ref = buf.at[source(z, d, ORDERS[d][k][0] + steps_more), rows_of(d, k), :]
        return pltpu.make_async_remote_copy(
            src_ref=ref, dst_ref=ref, send_sem=send_sem.at[d, k], recv_sem=recv_sem.at[d, k],
            device_id={"rows": to[d]}, device_id_type=MESH,
        )

    def gain_copy(d, hop, steps_more=0):
        ref = gains.at[c, source(z, d, hop + steps_more)]
        return pltpu.make_async_remote_copy(
            src_ref=ref, dst_ref=ref, send_sem=gsend.at[d, hop], recv_sem=grecv.at[d, hop],
            device_id={"rows": to[d]}, device_id_type=MESH,
        )

    def partner_copy(col):
        ref = gains.at[col]
        return pltpu.make_async_remote_copy(
            src_ref=ref, dst_ref=ref, send_sem=psend.at[0], recv_sem=precv.at[0],
            device_id={"cols": partner}, device_id_type=MESH,
        )

    def pair_copy(hop, steps_more=0):
        ref = gains.at[pl.ds(lax.rem(c - odd - 2 * (hop + steps_more) + N, N), 2)]
        return pltpu.make_async_remote_copy(
            src_ref=ref, dst_ref=ref, send_sem=psend.at[1 + hop], recv_sem=precv.at[1 + hop],
            device_id={"cols": up}, device_id_type=MESH,
        )

    def norm_step(k):
        hop = {2: 1, 3: 2, 5: 3}.get(k)
        for d in range(2):
            if hop is not None and hop < 4 - d:
                gain_copy(d, hop - 1, 1).wait_recv()
                gain_copy(d, hop).start()

    def norm_end():
        gain_copy(1, 2, 1).wait_recv()
        gain_copy(0, 3, 1).wait_recv()
        pl.when(odd == 1)(lambda: pl.semaphore_wait(ready.at[3], 1))
        partner_copy(c).start()
        partner_copy(partner).wait_recv()
        pl.when(c < N - 2)(lambda: pl.semaphore_wait(ready.at[2], 1))
        for hop in range(3):
            pair_copy(hop).start()
            pair_copy(hop, 1).wait_recv()
        lane = lax.broadcasted_iota(jnp.int32, (N, PAD), 1)
        rows = [jnp.zeros((N, PAD), F32) for _ in range(5)]
        for j in range(N):
            row, off = divmod(80 * j, PAD)
            v = gains[j].reshape(N, PAD)
            v = pltpu.roll(v, off, 1) if off else v
            rows[row] = jnp.where((lane >= off) & (lane < off + 80), v, rows[row])
            if off + 80 > PAD:
                rows[row + 1] = jnp.where(lane < off + 80 - PAD, v, rows[row + 1])
        for j in range(5):
            gain[pl.ds(j, N, stride=5), :] = rows[j]
        for d in range(2):
            for hop in range(4 - d):
                gain_copy(d, hop).wait_send()
        partner_copy(c).wait_send()
        for hop in range(3):
            pair_copy(hop).wait_send()

    def begin(d):
        greet(d)
        piece_copy(d, 0).start()

    def more(d):
        gain_copy(d, 0).start()
        piece_copy(d, 1).start()

    def share_norm():
        for x in got_norm:
            x.wait()
        gains[c, z, 0:1, 0:80] = (nt_v[...] + ns_v[...]).reshape(1, 80)

    @pl.when(z == 0)
    def _():
        begin(0)
        share_norm()
        for i in (5, 1, 4, 2, 3):
            compute(i)
        more(0)
        begin(1)
        more(1)

    @pl.when(z == N - 1)
    def _():
        begin(0)
        compute(5)
        begin(1)
        share_norm()
        for i in (1, 4, 2, 3):
            compute(i)
        more(0)
        more(1)

    @pl.when(jnp.logical_not(rightmost))
    def _():
        begin(1)
        compute(5)
        begin(0)
        share_norm()
        for i in (1, 4, 2, 3):
            compute(i)
        more(1)
        more(0)

    def item(k, met):
        for d in (1, 0):
            for i in needs(d, k):
                if (d, i) not in met:
                    piece_copy(d, i, 1).wait_recv()
                    met.add((d, i))
            piece_copy(d, k - DEPTH).wait_send()
            piece_copy(d, k).start()

    def drain(last, met):
        for d in range(2):
            for k in range(last - DEPTH, last):
                piece_copy(d, k).wait_send()
            for k in range(last):
                if (d, k) not in met:
                    piece_copy(d, k, 1).wait_recv()

    met = set()
    low = min(FIRST)
    for k in range(DEPTH, low):
        norm_step(k)
        item(k, met)
    norm_end()
    for parity in range(2):

        @pl.when(odd == parity)
        def _():
            mine = set(met)
            for k in range(low, FIRST[parity]):
                item(k, mine)
            drain(FIRST[parity], mine)


def finish(buf, late, send_sem, recv_sem):
    z = lax.axis_index("rows")
    odd = lax.rem(lax.axis_index("cols"), 2)
    to = (lax.rem(z + 1, N), lax.rem(z + N - 1, N))
    barrier = pltpu.get_barrier_semaphore()
    for d in range(2):
        pl.semaphore_signal(barrier, inc=1, device_id={"rows": to[d]}, device_id_type=MESH)
    pl.semaphore_wait(barrier, 2)

    def piece_copy(d, k, first):
        hop = ORDERS[d][k][0]
        here = late.at[d] if needs(d, k)[0] >= first else buf.at[source(z, d, hop)]
        return pltpu.make_async_remote_copy(
            src_ref=here.at[rows_of(d, k), :], dst_ref=late.at[2 if hop == 3 else d, rows_of(d, k), :],
            send_sem=send_sem.at[d, k], recv_sem=recv_sem.at[d, k],
            device_id={"rows": to[d]}, device_id_type=MESH,
        )

    for parity, first in enumerate(FIRST):

        @pl.when(odd == parity)
        def _():
            met = set()
            for k in range(first, NS):
                for d in (1, 0):
                    for i in needs(d, k):
                        if i >= first and (d, i) not in met:
                            piece_copy(d, i, first).wait_recv()
                            met.add((d, i))
                    if_sent(z, d, k, lambda d=d, k=k: piece_copy(d, k, first).start())
            for k in range(first, NS):
                for d in (1, 0):
                    if_sent(z, d, k, lambda d=d, k=k: piece_copy(d, k, first).wait_send())
                    if (d, k) not in met:
                        if_received(z, d, k, lambda d=d, k=k: piece_copy(d, k, first).wait_recv())


def write_out(outs, z, sem, blocks):
    copies = []
    for block, distance in blocks:
        at = pl.ds(pl.multiple_of(lax.rem(z + distance + N, N) * ROWS, ROWS), ROWS)
        first = 0
        for out, width in zip(outs, COLS):
            copies.append(pltpu.make_async_copy(block.at[pl.ds(first, width), :], out.at[:, at], sem.at[len(copies)]))
            first += width
    for copy in copies:
        copy.start()
    for copy in copies:
        copy.wait()


def early(parity):
    return (0, 1, -1, 2, -2) if FIRST[parity] == 7 else (0, 1, -1, 2, -2, 3, -3)


def deliver(buf, gain, q, k, v, g, sem):
    z = lax.axis_index("rows")
    odd = lax.rem(lax.axis_index("cols"), 2)
    g[...] = gain[...].astype(BF16)
    for parity in range(2):

        @pl.when(odd == parity)
        def _():
            write_out((q, k, v), z, sem, [(buf.at[lax.rem(z + b + N, N)], b) for b in early(parity)])


def deliver_late(late, q_in, k_in, v_in, q, k, v, sem):
    z = lax.axis_index("rows")
    odd = lax.rem(lax.axis_index("cols"), 2)
    for parity in range(2):

        @pl.when(odd == parity)
        def _():
            blocks = [(late.at[slot], b) for slot, b in enumerate((-3, 3, 4)) if b not in early(parity)]
            write_out((q, k, v), z, sem, blocks)


def local(wq, lq, hq, wk, lk, hk, wv, lv, hv, nt, ns):
    hbm = pl.BlockSpec(memory_space=pltpu.HBM)
    vmem = pl.BlockSpec(memory_space=pltpu.VMEM)
    dma = pltpu.SemaphoreType.DMA
    limit = 16 << 20
    args = (wq, lq.T, hq, wk, lk.T, hk, wv, lv.T, hv, nt, ns)
    buf, gain = pl.pallas_call(
        exchange,
        name="exchange",
        out_shape=(
            jax.ShapeDtypeStruct((N, WIDTH, ROWS), BF16),
            jax.ShapeDtypeStruct((40, PAD), F32),
        ),
        in_specs=[hbm] * 11,
        out_specs=(vmem, vmem),
        scratch_shapes=[
            pltpu.VMEM((5, ROWS, UNIT), BF16),
            pltpu.VMEM((ROWS, UNIT), BF16),
            pltpu.VMEM((ROWS, UNIT), BF16),
            pltpu.VMEM((32, ROWS), BF16),
            pltpu.VMEM((32, ROWS), BF16),
            pltpu.VMEM((32, ROWS), BF16),
            pltpu.VMEM((32, COLS[0]), BF16),
            pltpu.VMEM((32, COLS[1]), BF16),
            pltpu.VMEM((32, COLS[2]), BF16),
            pltpu.VMEM((80,), F32),
            pltpu.VMEM((80,), F32),
            pltpu.VMEM((N, N, 1, PAD), F32),
            dma((16,)),
            dma((2, NS)),
            dma((2, NS)),
            dma((2, 4)),
            dma((2, 4)),
            dma((4,)),
            dma((4,)),
            pltpu.SemaphoreType.REGULAR((4,)),
        ],
        compiler_params=pltpu.CompilerParams(collective_id=0, has_side_effects=True, vmem_limit_bytes=limit),
    )(*(pltpu.with_memory_space_constraint(x, pltpu.HBM) for x in args))
    wide = [jax.ShapeDtypeStruct((width, N * ROWS), BF16) for width in COLS]
    q, k, v, g = pl.pallas_call(
        deliver,
        name="deliver",
        out_shape=(*wide, jax.ShapeDtypeStruct((40, PAD), BF16)),
        in_specs=[vmem, vmem],
        out_specs=(hbm, hbm, hbm, vmem),
        scratch_shapes=[dma((32,))],
        compiler_params=pltpu.CompilerParams(vmem_limit_bytes=limit, has_side_effects=True),
    )(buf, gain)
    late = pl.pallas_call(
        finish,
        name="finish",
        out_shape=jax.ShapeDtypeStruct((3, WIDTH, ROWS), BF16),
        in_specs=[vmem],
        out_specs=vmem,
        scratch_shapes=[dma((2, NS)), dma((2, NS))],
        compiler_params=pltpu.CompilerParams(collective_id=1, has_side_effects=True, vmem_limit_bytes=limit),
    )(buf)
    q, k, v = pl.pallas_call(
        deliver_late,
        name="deliver_late",
        out_shape=tuple(wide),
        in_specs=[vmem, hbm, hbm, hbm],
        out_specs=(hbm, hbm, hbm),
        scratch_shapes=[dma((16,))],
        input_output_aliases={1: 0, 2: 1, 3: 2},
        compiler_params=pltpu.CompilerParams(vmem_limit_bytes=limit),
    )(late, q, k, v)
    return q, k, v, g.reshape(N * ROWS)


def solution(mesh):
    return jax.shard_map(
        local,
        mesh=mesh,
        in_specs=(
            P(("trial", "rows"), "cols"),
            P(("trial", "rows"), None),
            P("trial", "cols"),
            P(("trial", "rows"), "cols"),
            P(("trial", "rows"), None),
            P("trial", "cols"),
            P(("trial", "rows"), "cols"),
            P(("trial", "rows"), None),
            P("trial", "cols"),
            P(("trial", "rows", "cols")),
            P(("trial", "rows", "cols")),
        ),
        out_specs=(
            P(("trial", "cols"), None),
            P(("trial", "cols"), None),
            P(("trial", "cols"), None),
            P("trial"),
        ),
        check_vma=False,
    )
```

```python
import functools

import jax
import jax.numpy as jnp
from jax import lax
from jax.experimental import pallas as pl
from jax.experimental.pallas import tpu as pltpu
from jax.sharding import PartitionSpec as P

MESH = pl.DeviceIdType.MESH
MIX = 2.0
F32 = jnp.float32
BF16 = jnp.bfloat16

N = 8
ROWS = 640
COLS = (640, 128, 128)
WIDTH = sum(COLS)
PAD = 128
UNIT = 128
HOPS = (
    ((0, 128), (128, 320), (448, 448)),
    ((0, 448), (448, 448)),
    ((0, 448), (448, 448)),
    ((0, 384), (384, 64)),
)
RIGHT = [(h, *piece) for h, pieces in enumerate(HOPS) for piece in pieces]
LEFT = [(h, WIDTH - first - height, height) for h, first, height in RIGHT[:-2]] + [(3, 448, 448), (3, 384, 64)]
ORDERS = (RIGHT, LEFT)
NS = len(RIGHT)
LAST = NS - 1
DEPTH = 2
FIRST = (7, 5)
SIGN = (1, -1)


def source(z, d, steps):
    return lax.rem(z - SIGN[d] * steps + N, N)


def rows_of(d, k):
    return pl.ds(*ORDERS[d][k][1:])


def needs(d, k):
    hop, first, height = ORDERS[d][k]
    return [
        i for i, (h, f, n) in enumerate(ORDERS[d])
        if h == hop - 1 and f < first + height and first < f + n
    ]


def if_sent(z, d, k, act):
    if k < LAST:
        act()
    else:
        pl.when(z < N - 1 if d == 0 else z == 1)(act)


def if_received(z, d, k, act):
    if k < LAST:
        act()
    else:
        pl.when(z > 0 if d == 0 else z == 0)(act)


def exchange(
    wq, lq, hq, wk, lk, hk, wv, lv, hv, nt, ns,
    buf, gain,
    wq_v, wk_v, wv_v, lq_v, lk_v, lv_v, hq_v, hk_v, hv_v, nt_v, ns_v, gains,
    in_sem, send_sem, recv_sem, gsend, grecv, psend, precv, ready,
):
    z = lax.axis_index("rows")
    c = lax.axis_index("cols")
    to = (lax.rem(z + 1, N), lax.rem(z + N - 1, N))
    up, down = lax.rem(c + 2, N), lax.rem(c + N - 2, N)
    odd = lax.rem(c, 2)
    partner = c + 1 - 2 * odd
    barrier = pltpu.get_barrier_semaphore()

    def signal(sem, **who):
        pl.semaphore_signal(sem, inc=1, device_id=who, device_id_type=MESH)

    pl.when(z < N - 1)(lambda: signal(barrier, rows=to[0]))
    pl.when(z == 0)(lambda: signal(barrier, rows=to[1]))
    pl.when(c < N - 2)(lambda: signal(barrier, cols=up))
    pl.when(c < 2)(lambda: signal(barrier, cols=down))
    pl.when(odd == 1)(lambda: signal(barrier, cols=partner))

    count = [0]

    def load(src, dst):
        copy = pltpu.make_async_copy(src, dst, in_sem.at[count[0]])
        copy.start()
        count[0] += 1
        return copy

    got = {6: [load(lv, lv_v), load(hv, hv_v), load(wv, wv_v)]}
    got[0] = [load(lq, lq_v), load(hq, hq_v), load(wq.at[:, pl.ds(0, UNIT)], wq_v.at[0])]
    got_norm = [load(nt, nt_v), load(ns, ns_v)]
    got[5] = [load(lk, lk_v), load(hk, hk_v), load(wk, wk_v)]
    for i in (1, 4, 2, 3):
        got[i] = [load(wq.at[:, pl.ds(i * UNIT, UNIT)], wq_v.at[i])]

    def greet(d):
        pl.when(z < N - 1 if d == 0 else z == 0)(lambda: pl.semaphore_wait(ready.at[d], 1))

    def compute(i):
        for x in got[i]:
            x.wait()
        w, h, lt = (
            (wq_v[i], hq_v[:, i * UNIT : (i + 1) * UNIT], lq_v[...]) if i < 5
            else (wk_v[...], hk_v[...], lk_v[...]) if i == 5
            else (wv_v[...], hv_v[...], lv_v[...])
        )
        delta = lax.dot_general(h, lt, (((0,), (0,)), ((), ())), preferred_element_type=F32)
        buf[z, pl.ds(i * UNIT, UNIT), :] = (w.T.astype(F32) + MIX * delta).astype(BF16)

    rightmost = (z == 0) | (z == N - 1)

    @pl.when(rightmost)
    def _():
        compute(0)
        compute(6)

    @pl.when(jnp.logical_not(rightmost))
    def _():
        compute(6)
        compute(0)

    for x in got_norm:
        x.wait()
    gains[c, z, 0:1, 0:80] = (nt_v[...] + ns_v[...]).reshape(1, 80)

    ahead = [z > 0, z == N - 1, c >= 2, c >= N - 2, odd == 0]
    ahead = sum(x.astype(jnp.int32) for x in ahead)
    pl.when(ahead > 0)(lambda: pl.semaphore_wait(barrier, ahead))
    pl.when(z > 0)(lambda: signal(ready.at[0], rows=to[1]))
    pl.when(z == N - 1)(lambda: signal(ready.at[1], rows=to[0]))
    pl.when(c >= 2)(lambda: signal(ready.at[2], cols=down))
    pl.when(odd == 0)(lambda: signal(ready.at[3], cols=partner))

    def piece_copy(d, k, steps_more=0):
        ref = buf.at[source(z, d, ORDERS[d][k][0] + steps_more), rows_of(d, k), :]
        return pltpu.make_async_remote_copy(
            src_ref=ref, dst_ref=ref, send_sem=send_sem.at[d, k], recv_sem=recv_sem.at[d, k],
            device_id={"rows": to[d]}, device_id_type=MESH,
        )

    def gain_copy(d, hop, steps_more=0):
        ref = gains.at[c, source(z, d, hop + steps_more)]
        return pltpu.make_async_remote_copy(
            src_ref=ref, dst_ref=ref, send_sem=gsend.at[d, hop], recv_sem=grecv.at[d, hop],
            device_id={"rows": to[d]}, device_id_type=MESH,
        )

    def partner_copy(col):
        ref = gains.at[col]
        return pltpu.make_async_remote_copy(
            src_ref=ref, dst_ref=ref, send_sem=psend.at[0], recv_sem=precv.at[0],
            device_id={"cols": partner}, device_id_type=MESH,
        )

    def pair_copy(hop, steps_more=0):
        ref = gains.at[pl.ds(lax.rem(c - odd - 2 * (hop + steps_more) + N, N), 2)]
        return pltpu.make_async_remote_copy(
            src_ref=ref, dst_ref=ref, send_sem=psend.at[1 + hop], recv_sem=precv.at[1 + hop],
            device_id={"cols": up}, device_id_type=MESH,
        )

    def norm_step(k):
        hop = {2: 1, 3: 2, 4: 3}.get(k)
        for d in range(2):
            if hop is not None and hop < 4 - d:
                gain_copy(d, hop - 1, 1).wait_recv()
                gain_copy(d, hop).start()

    def norm_end():
        gain_copy(1, 2, 1).wait_recv()
        gain_copy(0, 3, 1).wait_recv()
        pl.when(odd == 1)(lambda: pl.semaphore_wait(ready.at[3], 1))
        partner_copy(c).start()
        partner_copy(partner).wait_recv()
        pl.when(c < N - 2)(lambda: pl.semaphore_wait(ready.at[2], 1))
        for hop in range(3):
            pair_copy(hop).start()
            pair_copy(hop, 1).wait_recv()
        lane = lax.broadcasted_iota(jnp.int32, (N, PAD), 1)
        rows = [jnp.zeros((N, PAD), F32) for _ in range(5)]
        for j in range(N):
            row, off = divmod(80 * j, PAD)
            v = gains[j].reshape(N, PAD)
            v = pltpu.roll(v, off, 1) if off else v
            rows[row] = jnp.where((lane >= off) & (lane < off + 80), v, rows[row])
            if off + 80 > PAD:
                rows[row + 1] = jnp.where(lane < off + 80 - PAD, v, rows[row + 1])
        for j in range(5):
            gain[pl.ds(j, N, stride=5), :] = rows[j]
        for d in range(2):
            for hop in range(4 - d):
                gain_copy(d, hop).wait_send()
        partner_copy(c).wait_send()
        for hop in range(3):
            pair_copy(hop).wait_send()

    def begin(d):
        greet(d)
        gain_copy(d, 0).start()
        piece_copy(d, 0).start()

    def second(*ways):
        for d in ways:
            piece_copy(d, 1).start()

    @pl.when(z == 0)
    def _():
        begin(0)
        for i in (5, 1, 4, 2, 3):
            compute(i)
        second(0)
        begin(1)
        second(1)

    @pl.when(z == N - 1)
    def _():
        begin(0)
        compute(5)
        begin(1)
        for i in (1, 4, 2, 3):
            compute(i)
        second(0, 1)

    @pl.when(jnp.logical_not(rightmost))
    def _():
        begin(1)
        compute(5)
        begin(0)
        for i in (1, 4, 2, 3):
            compute(i)
        second(1, 0)

    def item(k, met):
        for d in (1, 0):
            for i in needs(d, k):
                if (d, i) not in met:
                    piece_copy(d, i, 1).wait_recv()
                    met.add((d, i))
            piece_copy(d, k - DEPTH).wait_send()
            piece_copy(d, k).start()

    def drain(last, met):
        for d in range(2):
            for k in range(last - DEPTH, last):
                piece_copy(d, k).wait_send()
            for k in range(last):
                if (d, k) not in met:
                    piece_copy(d, k, 1).wait_recv()

    met = set()
    low = min(FIRST)
    for k in range(DEPTH, low):
        norm_step(k)
        item(k, met)
    for parity in range(2):

        @pl.when(odd == parity)
        def _():
            mine = set(met)
            for k in range(low, FIRST[parity]):
                item(k, mine)
                if k == low:
                    norm_end()
            if FIRST[parity] == low:
                norm_end()
            drain(FIRST[parity], mine)


def finish(buf, late, send_sem, recv_sem):
    z = lax.axis_index("rows")
    odd = lax.rem(lax.axis_index("cols"), 2)
    to = (lax.rem(z + 1, N), lax.rem(z + N - 1, N))
    barrier = pltpu.get_barrier_semaphore()
    for d in range(2):
        pl.semaphore_signal(barrier, inc=1, device_id={"rows": to[d]}, device_id_type=MESH)
    pl.semaphore_wait(barrier, 2)

    def piece_copy(d, k, first):
        hop = ORDERS[d][k][0]
        here = late.at[d] if needs(d, k)[0] >= first else buf.at[source(z, d, hop)]
        return pltpu.make_async_remote_copy(
            src_ref=here.at[rows_of(d, k), :], dst_ref=late.at[2 if hop == 3 else d, rows_of(d, k), :],
            send_sem=send_sem.at[d, k], recv_sem=recv_sem.at[d, k],
            device_id={"rows": to[d]}, device_id_type=MESH,
        )

    for parity, first in enumerate(FIRST):

        @pl.when(odd == parity)
        def _():
            met = set()
            for k in range(first, NS):
                for d in (1, 0):
                    for i in needs(d, k):
                        if i >= first and (d, i) not in met:
                            piece_copy(d, i, first).wait_recv()
                            met.add((d, i))
                    if_sent(z, d, k, lambda d=d, k=k: piece_copy(d, k, first).start())
            for k in range(first, NS):
                for d in (1, 0):
                    if_sent(z, d, k, lambda d=d, k=k: piece_copy(d, k, first).wait_send())
                    if (d, k) not in met:
                        if_received(z, d, k, lambda d=d, k=k: piece_copy(d, k, first).wait_recv())


def write_out(outs, z, sem, blocks):
    copies = []
    for block, distance in blocks:
        at = pl.ds(pl.multiple_of(lax.rem(z + distance + N, N) * ROWS, ROWS), ROWS)
        first = 0
        for out, width in zip(outs, COLS):
            copies.append(pltpu.make_async_copy(block.at[pl.ds(first, width), :], out.at[:, at], sem.at[len(copies)]))
            first += width
    for copy in copies:
        copy.start()
    for copy in copies:
        copy.wait()


def early(parity):
    return (0, 1, -1, 2, -2) if FIRST[parity] == 5 else (0, 1, -1, 2, -2, 3, -3)


def deliver(buf, gain, q, k, v, g, sem):
    z = lax.axis_index("rows")
    odd = lax.rem(lax.axis_index("cols"), 2)
    g[...] = gain[...].astype(BF16)
    for parity in range(2):

        @pl.when(odd == parity)
        def _():
            write_out((q, k, v), z, sem, [(buf.at[lax.rem(z + b + N, N)], b) for b in early(parity)])


def deliver_late(late, q_in, k_in, v_in, q, k, v, sem):
    z = lax.axis_index("rows")
    odd = lax.rem(lax.axis_index("cols"), 2)
    for parity in range(2):

        @pl.when(odd == parity)
        def _():
            blocks = [(late.at[slot], b) for slot, b in enumerate((-3, 3, 4)) if b not in early(parity)]
            write_out((q, k, v), z, sem, blocks)


def local(wq, lq, hq, wk, lk, hk, wv, lv, hv, nt, ns):
    hbm = pl.BlockSpec(memory_space=pltpu.HBM)
    vmem = pl.BlockSpec(memory_space=pltpu.VMEM)
    dma = pltpu.SemaphoreType.DMA
    limit = 16 << 20
    args = (wq, lq.T, hq, wk, lk.T, hk, wv, lv.T, hv, nt, ns)
    buf, gain = pl.pallas_call(
        exchange,
        name="exchange",
        out_shape=(
            jax.ShapeDtypeStruct((N, WIDTH, ROWS), BF16),
            jax.ShapeDtypeStruct((40, PAD), F32),
        ),
        in_specs=[hbm] * 11,
        out_specs=(vmem, vmem),
        scratch_shapes=[
            pltpu.VMEM((5, ROWS, UNIT), BF16),
            pltpu.VMEM((ROWS, UNIT), BF16),
            pltpu.VMEM((ROWS, UNIT), BF16),
            pltpu.VMEM((32, ROWS), BF16),
            pltpu.VMEM((32, ROWS), BF16),
            pltpu.VMEM((32, ROWS), BF16),
            pltpu.VMEM((32, COLS[0]), BF16),
            pltpu.VMEM((32, COLS[1]), BF16),
            pltpu.VMEM((32, COLS[2]), BF16),
            pltpu.VMEM((80,), F32),
            pltpu.VMEM((80,), F32),
            pltpu.VMEM((N, N, 1, PAD), F32),
            dma((16,)),
            dma((2, NS)),
            dma((2, NS)),
            dma((2, 4)),
            dma((2, 4)),
            dma((4,)),
            dma((4,)),
            pltpu.SemaphoreType.REGULAR((4,)),
        ],
        compiler_params=pltpu.CompilerParams(collective_id=0, has_side_effects=True, vmem_limit_bytes=limit),
    )(*(pltpu.with_memory_space_constraint(x, pltpu.HBM) for x in args))
    wide = [jax.ShapeDtypeStruct((width, N * ROWS), BF16) for width in COLS]
    q, k, v, g = pl.pallas_call(
        deliver,
        name="deliver",
        out_shape=(*wide, jax.ShapeDtypeStruct((40, PAD), BF16)),
        in_specs=[vmem, vmem],
        out_specs=(hbm, hbm, hbm, vmem),
        scratch_shapes=[dma((32,))],
        compiler_params=pltpu.CompilerParams(vmem_limit_bytes=limit, has_side_effects=True),
    )(buf, gain)
    late = pl.pallas_call(
        finish,
        name="finish",
        out_shape=jax.ShapeDtypeStruct((3, WIDTH, ROWS), BF16),
        in_specs=[vmem],
        out_specs=vmem,
        scratch_shapes=[dma((2, NS)), dma((2, NS))],
        compiler_params=pltpu.CompilerParams(collective_id=1, has_side_effects=True, vmem_limit_bytes=limit),
    )(buf)
    q, k, v = pl.pallas_call(
        deliver_late,
        name="deliver_late",
        out_shape=tuple(wide),
        in_specs=[vmem, hbm, hbm, hbm],
        out_specs=(hbm, hbm, hbm),
        scratch_shapes=[dma((16,))],
        input_output_aliases={1: 0, 2: 1, 3: 2},
        compiler_params=pltpu.CompilerParams(vmem_limit_bytes=limit),
    )(late, q, k, v)
    return q, k, v, g.reshape(N * ROWS)


def solution(mesh):
    return jax.shard_map(
        local,
        mesh=mesh,
        in_specs=(
            P(("trial", "rows"), "cols"),
            P(("trial", "rows"), None),
            P("trial", "cols"),
            P(("trial", "rows"), "cols"),
            P(("trial", "rows"), None),
            P("trial", "cols"),
            P(("trial", "rows"), "cols"),
            P(("trial", "rows"), None),
            P("trial", "cols"),
            P(("trial", "rows", "cols")),
            P(("trial", "rows", "cols")),
        ),
        out_specs=(
            P(("trial", "cols"), None),
            P(("trial", "cols"), None),
            P(("trial", "cols"), None),
            P("trial"),
        ),
        check_vma=False,
    )
```

```python
import functools

import jax
import jax.numpy as jnp
from jax import lax
from jax.experimental import pallas as pl
from jax.experimental.pallas import tpu as pltpu
from jax.sharding import PartitionSpec as P

MESH = pl.DeviceIdType.MESH
MIX = 2.0
F32 = jnp.float32
BF16 = jnp.bfloat16

N = 8
ROWS = 640
COLS = (640, 128, 128)
WIDTH = sum(COLS)
PAD = 128
UNIT = 128
HOPS = (
    ((0, 128), (128, 320), (448, 448)),
    ((0, 448), (448, 448)),
    ((0, 448), (448, 448)),
    ((0, 368), (368, 80)),
)
RIGHT = [(h, *piece) for h, pieces in enumerate(HOPS) for piece in pieces]
LEFT = [(h, WIDTH - first - height, height) for h, first, height in RIGHT[:-2]] + [(3, 448, 448), (3, 368, 80)]
ORDERS = (RIGHT, LEFT)
NS = len(RIGHT)
LAST = NS - 1
DEPTH = 2
FIRST = (7, 5)
SIGN = (1, -1)


def wrapped(x):
    return x + N * (x < 0).astype(jnp.int32) - N * (x >= N).astype(jnp.int32)


def source(z, d, steps):
    return wrapped(z - SIGN[d] * steps)


def rows_of(d, k):
    return pl.ds(*ORDERS[d][k][1:])


def needs(d, k):
    hop, first, height = ORDERS[d][k]
    return [
        i for i, (h, f, n) in enumerate(ORDERS[d])
        if h == hop - 1 and f < first + height and first < f + n
    ]


def if_sent(z, d, k, act):
    if k < LAST:
        act()
    else:
        pl.when(z < N - 1 if d == 0 else z == 1)(act)


def if_received(z, d, k, act):
    if k < LAST:
        act()
    else:
        pl.when(z > 0 if d == 0 else z == 0)(act)


def exchange(
    wq, lq, hq, wk, lk, hk, wv, lv, hv, nt, ns,
    buf, gain,
    wq_v, wk_v, wv_v, lq_v, lk_v, lv_v, hq_v, hk_v, hv_v, nt_v, ns_v, gains,
    in_sem, send_sem, recv_sem, gsend, grecv, psend, precv, ready,
):
    count = [0]

    def load(src, dst):
        copy = pltpu.make_async_copy(src, dst, in_sem.at[count[0]])
        copy.start()
        count[0] += 1
        return copy

    got = {6: [load(lv, lv_v), load(hv, hv_v), load(wv, wv_v)]}
    got[0] = [load(lq, lq_v), load(hq, hq_v), load(wq.at[:, pl.ds(0, UNIT)], wq_v.at[0])]
    got_norm = [load(nt, nt_v), load(ns, ns_v)]
    got[5] = [load(lk, lk_v), load(hk, hk_v), load(wk, wk_v)]
    for i in (1, 4, 2, 3):
        got[i] = [load(wq.at[:, pl.ds(i * UNIT, UNIT)], wq_v.at[i])]

    z = lax.axis_index("rows")
    c = lax.axis_index("cols")
    to = (wrapped(z + 1), wrapped(z - 1))
    up, down = wrapped(c + 2), wrapped(c - 2)
    odd = lax.rem(c, 2)
    partner = c + 1 - 2 * odd
    barrier = pltpu.get_barrier_semaphore()

    def signal(sem, **who):
        pl.semaphore_signal(sem, inc=1, device_id=who, device_id_type=MESH)

    pl.when(z < N - 2)(lambda: signal(barrier, rows=to[0]))
    pl.when((z == 0) | (z == N - 1))(lambda: signal(barrier, rows=to[1]))
    pl.when(c < N - 2)(lambda: signal(barrier, cols=up))
    pl.when(c < 2)(lambda: signal(barrier, cols=down))
    pl.when(odd == 1)(lambda: signal(barrier, cols=partner))

    def greet(d):
        pl.when(z < N - 2 if d == 0 else rightmost)(lambda: pl.semaphore_wait(ready.at[d], 1))

    def compute(i):
        for x in got[i]:
            x.wait()
        w, h, lt = (
            (wq_v[i], hq_v[:, i * UNIT : (i + 1) * UNIT], lq_v[...]) if i < 5
            else (wk_v[...], hk_v[...], lk_v[...]) if i == 5
            else (wv_v[...], hv_v[...], lv_v[...])
        )
        delta = lax.dot_general(h, lt, (((0,), (0,)), ((), ())), preferred_element_type=F32)
        buf[z, pl.ds(i * UNIT, UNIT), :] = (w.T.astype(F32) + MIX * delta).astype(BF16)

    ahead = [(z > 0) & (z < N - 1), z >= N - 2, c >= 2, c >= N - 2, odd == 0]
    ahead = sum(x.astype(jnp.int32) for x in ahead)
    pl.when(ahead > 0)(lambda: pl.semaphore_wait(barrier, ahead))
    pl.when((z > 0) & (z < N - 1))(lambda: signal(ready.at[0], rows=to[1]))
    pl.when(z >= N - 2)(lambda: signal(ready.at[1], rows=to[0]))
    pl.when(c >= 2)(lambda: signal(ready.at[2], cols=down))
    pl.when(odd == 0)(lambda: signal(ready.at[3], cols=partner))

    rightmost = (z == 0) | (z == N - 1)

    @pl.when(rightmost)
    def _():
        compute(0)
        compute(6)

    @pl.when(jnp.logical_not(rightmost))
    def _():
        compute(6)
        compute(0)

    for x in got_norm:
        x.wait()
    gains[c, z, 0:1, 0:80] = (nt_v[...] + ns_v[...]).reshape(1, 80)

    def piece_copy(d, k, steps_more=0):
        ref = buf.at[source(z, d, ORDERS[d][k][0] + steps_more), rows_of(d, k), :]
        return pltpu.make_async_remote_copy(
            src_ref=ref, dst_ref=ref, send_sem=send_sem.at[d, k], recv_sem=recv_sem.at[d, k],
            device_id={"rows": to[d]}, device_id_type=MESH,
        )

    def gain_copy(d, hop, steps_more=0):
        ref = gains.at[c, source(z, d, hop + steps_more)]
        return pltpu.make_async_remote_copy(
            src_ref=ref, dst_ref=ref, send_sem=gsend.at[d, hop], recv_sem=grecv.at[d, hop],
            device_id={"rows": to[d]}, device_id_type=MESH,
        )

    def partner_copy(col):
        ref = gains.at[col]
        return pltpu.make_async_remote_copy(
            src_ref=ref, dst_ref=ref, send_sem=psend.at[0], recv_sem=precv.at[0],
            device_id={"cols": partner}, device_id_type=MESH,
        )

    def pair_copy(hop, steps_more=0):
        ref = gains.at[pl.ds(wrapped(c - odd - 2 * (hop + steps_more)), 2)]
        return pltpu.make_async_remote_copy(
            src_ref=ref, dst_ref=ref, send_sem=psend.at[1 + hop], recv_sem=precv.at[1 + hop],
            device_id={"cols": up}, device_id_type=MESH,
        )

    def norm_step(k):
        hop = {2: 1, 3: 2, 4: 3}.get(k)
        for d in range(2):
            if hop is not None and hop < 4 - d:
                gain_copy(d, hop - 1, 1).wait_recv()
                gain_copy(d, hop).start()

    def norm_end():
        gain_copy(1, 2, 1).wait_recv()
        gain_copy(0, 3, 1).wait_recv()
        pl.when(odd == 1)(lambda: pl.semaphore_wait(ready.at[3], 1))
        partner_copy(c).start()
        partner_copy(partner).wait_recv()
        pl.when(c < N - 2)(lambda: pl.semaphore_wait(ready.at[2], 1))
        for hop in range(3):
            pair_copy(hop).start()
            pair_copy(hop, 1).wait_recv()
        lane = lax.broadcasted_iota(jnp.int32, (N, PAD), 1)
        rows = [jnp.zeros((N, PAD), F32) for _ in range(5)]
        for j in range(N):
            row, off = divmod(80 * j, PAD)
            v = gains[j].reshape(N, PAD)
            v = pltpu.roll(v, off, 1) if off else v
            rows[row] = jnp.where((lane >= off) & (lane < off + 80), v, rows[row])
            if off + 80 > PAD:
                rows[row + 1] = jnp.where(lane < off + 80 - PAD, v, rows[row + 1])
        for j in range(5):
            gain[pl.ds(j, N, stride=5), :] = rows[j]
        for d in range(2):
            for hop in range(4 - d):
                gain_copy(d, hop).wait_send()
        partner_copy(c).wait_send()
        for hop in range(3):
            pair_copy(hop).wait_send()

    def begin(d):
        greet(d)
        gain_copy(d, 0).start()
        piece_copy(d, 0).start()

    def second(*ways):
        for d in ways:
            piece_copy(d, 1).start()

    @pl.when(z == 0)
    def _():
        begin(0)
        for i in (5, 1, 4, 2, 3):
            compute(i)
        second(0)
        begin(1)
        second(1)

    @pl.when(z == N - 1)
    def _():
        begin(0)
        compute(5)
        begin(1)
        for i in (1, 4, 2, 3):
            compute(i)
        second(0, 1)

    @pl.when(jnp.logical_not(rightmost))
    def _():
        begin(1)
        compute(5)
        begin(0)
        for i in (1, 4, 2, 3):
            compute(i)
        second(1, 0)

    def item(k, met):
        for d in (1, 0):
            for i in needs(d, k):
                if (d, i) not in met:
                    piece_copy(d, i, 1).wait_recv()
                    met.add((d, i))
            piece_copy(d, k - DEPTH).wait_send()
            piece_copy(d, k).start()

    def drain(last, met):
        for d in range(2):
            for k in range(last - DEPTH, last):
                piece_copy(d, k).wait_send()
            for k in range(last):
                if (d, k) not in met:
                    piece_copy(d, k, 1).wait_recv()

    met = set()
    low = min(FIRST)
    for k in range(DEPTH, low):
        norm_step(k)
        item(k, met)
    for parity in range(2):

        @pl.when(odd == parity)
        def _():
            mine = set(met)
            for k in range(low, FIRST[parity]):
                item(k, mine)
                if k == low:
                    norm_end()
            if FIRST[parity] == low:
                norm_end()
            drain(FIRST[parity], mine)


def finish(buf, late, send_sem, recv_sem):
    z = lax.axis_index("rows")
    odd = lax.rem(lax.axis_index("cols"), 2)
    to = (wrapped(z + 1), wrapped(z - 1))
    barrier = pltpu.get_barrier_semaphore()
    for d in range(2):
        pl.semaphore_signal(barrier, inc=1, device_id={"rows": to[d]}, device_id_type=MESH)
    pl.semaphore_wait(barrier, 2)

    def piece_copy(d, k, first):
        hop = ORDERS[d][k][0]
        here = late.at[d] if needs(d, k)[0] >= first else buf.at[source(z, d, hop)]
        return pltpu.make_async_remote_copy(
            src_ref=here.at[rows_of(d, k), :], dst_ref=late.at[2 if hop == 3 else d, rows_of(d, k), :],
            send_sem=send_sem.at[d, k], recv_sem=recv_sem.at[d, k],
            device_id={"rows": to[d]}, device_id_type=MESH,
        )

    for parity, first in enumerate(FIRST):

        @pl.when(odd == parity)
        def _():
            met = set()
            for k in range(first, NS):
                for d in (1, 0):
                    for i in needs(d, k):
                        if i >= first and (d, i) not in met:
                            piece_copy(d, i, first).wait_recv()
                            met.add((d, i))
                    if_sent(z, d, k, lambda d=d, k=k: piece_copy(d, k, first).start())
            for k in range(first, NS):
                for d in (1, 0):
                    if_sent(z, d, k, lambda d=d, k=k: piece_copy(d, k, first).wait_send())
                    if (d, k) not in met:
                        if_received(z, d, k, lambda d=d, k=k: piece_copy(d, k, first).wait_recv())


def write_out(outs, z, sem, blocks):
    copies = []
    for block, distance in blocks:
        at = pl.ds(pl.multiple_of(wrapped(z + distance) * ROWS, ROWS), ROWS)
        first = 0
        for out, width in zip(outs, COLS):
            copies.append(pltpu.make_async_copy(block.at[pl.ds(first, width), :], out.at[:, at], sem.at[len(copies)]))
            first += width
    for copy in copies:
        copy.start()
    for copy in copies:
        copy.wait()


def early(parity):
    return (0, 1, -1, 2, -2) if FIRST[parity] == 5 else (0, 1, -1, 2, -2, 3, -3)


def deliver(buf, gain, q, k, v, g, sem):
    z = lax.axis_index("rows")
    odd = lax.rem(lax.axis_index("cols"), 2)
    g[...] = gain[...].astype(BF16)
    for parity in range(2):

        @pl.when(odd == parity)
        def _():
            write_out((q, k, v), z, sem, [(buf.at[wrapped(z + b)], b) for b in early(parity)])


def deliver_late(late, q_in, k_in, v_in, q, k, v, sem):
    z = lax.axis_index("rows")
    odd = lax.rem(lax.axis_index("cols"), 2)
    for parity in range(2):

        @pl.when(odd == parity)
        def _():
            blocks = [(late.at[slot], b) for slot, b in enumerate((-3, 3, 4)) if b not in early(parity)]
            write_out((q, k, v), z, sem, blocks)


def local(wq, lq, hq, wk, lk, hk, wv, lv, hv, nt, ns):
    hbm = pl.BlockSpec(memory_space=pltpu.HBM)
    vmem = pl.BlockSpec(memory_space=pltpu.VMEM)
    dma = pltpu.SemaphoreType.DMA
    limit = 16 << 20
    args = (wq, lq.T, hq, wk, lk.T, hk, wv, lv.T, hv, nt, ns)
    buf, gain = pl.pallas_call(
        exchange,
        name="exchange",
        out_shape=(
            jax.ShapeDtypeStruct((N, WIDTH, ROWS), BF16),
            jax.ShapeDtypeStruct((40, PAD), F32),
        ),
        in_specs=[hbm] * 11,
        out_specs=(vmem, vmem),
        scratch_shapes=[
            pltpu.VMEM((5, ROWS, UNIT), BF16),
            pltpu.VMEM((ROWS, UNIT), BF16),
            pltpu.VMEM((ROWS, UNIT), BF16),
            pltpu.VMEM((32, ROWS), BF16),
            pltpu.VMEM((32, ROWS), BF16),
            pltpu.VMEM((32, ROWS), BF16),
            pltpu.VMEM((32, COLS[0]), BF16),
            pltpu.VMEM((32, COLS[1]), BF16),
            pltpu.VMEM((32, COLS[2]), BF16),
            pltpu.VMEM((80,), F32),
            pltpu.VMEM((80,), F32),
            pltpu.VMEM((N, N, 1, PAD), F32),
            dma((16,)),
            dma((2, NS)),
            dma((2, NS)),
            dma((2, 4)),
            dma((2, 4)),
            dma((4,)),
            dma((4,)),
            pltpu.SemaphoreType.REGULAR((4,)),
        ],
        compiler_params=pltpu.CompilerParams(collective_id=0, has_side_effects=True, vmem_limit_bytes=limit),
    )(*(pltpu.with_memory_space_constraint(x, pltpu.HBM) for x in args))
    wide = [jax.ShapeDtypeStruct((width, N * ROWS), BF16) for width in COLS]
    q, k, v, g = pl.pallas_call(
        deliver,
        name="deliver",
        out_shape=(*wide, jax.ShapeDtypeStruct((40, PAD), BF16)),
        in_specs=[vmem, vmem],
        out_specs=(hbm, hbm, hbm, vmem),
        scratch_shapes=[dma((32,))],
        compiler_params=pltpu.CompilerParams(vmem_limit_bytes=limit, has_side_effects=True),
    )(buf, gain)
    late = pl.pallas_call(
        finish,
        name="finish",
        out_shape=jax.ShapeDtypeStruct((3, WIDTH, ROWS), BF16),
        in_specs=[vmem],
        out_specs=vmem,
        scratch_shapes=[dma((2, NS)), dma((2, NS))],
        compiler_params=pltpu.CompilerParams(collective_id=1, has_side_effects=True, vmem_limit_bytes=limit),
    )(buf)
    q, k, v = pl.pallas_call(
        deliver_late,
        name="deliver_late",
        out_shape=tuple(wide),
        in_specs=[vmem, hbm, hbm, hbm],
        out_specs=(hbm, hbm, hbm),
        scratch_shapes=[dma((16,))],
        input_output_aliases={1: 0, 2: 1, 3: 2},
        compiler_params=pltpu.CompilerParams(vmem_limit_bytes=limit),
    )(late, q, k, v)
    return q, k, v, g.reshape(N * ROWS)


def solution(mesh):
    return jax.shard_map(
        local,
        mesh=mesh,
        in_specs=(
            P(("trial", "rows"), "cols"),
            P(("trial", "rows"), None),
            P("trial", "cols"),
            P(("trial", "rows"), "cols"),
            P(("trial", "rows"), None),
            P("trial", "cols"),
            P(("trial", "rows"), "cols"),
            P(("trial", "rows"), None),
            P("trial", "cols"),
            P(("trial", "rows", "cols")),
            P(("trial", "rows", "cols")),
        ),
        out_specs=(
            P(("trial", "cols"), None),
            P(("trial", "cols"), None),
            P(("trial", "cols"), None),
            P("trial"),
        ),
        check_vma=False,
    )
```

```python
import functools

import jax
import jax.numpy as jnp
from jax import lax
from jax.experimental import pallas as pl
from jax.experimental.pallas import tpu as pltpu
from jax.sharding import PartitionSpec as P

MESH = pl.DeviceIdType.MESH
MIX = 2.0
F32 = jnp.float32
BF16 = jnp.bfloat16

N = 8
ROWS = 640
COLS = (640, 128, 128)
WIDTH = sum(COLS)
PAD = 128
UNIT = 128
HOPS = (
    ((0, 128), (128, 320), (448, 448)),
    ((0, 448), (448, 448)),
    ((0, 448), (448, 448)),
    ((0, 368), (368, 80)),
)
RIGHT = [(h, *piece) for h, pieces in enumerate(HOPS) for piece in pieces]
LEFT = [(h, WIDTH - first - height, height) for h, first, height in RIGHT[:-2]] + [(3, 448, 448), (3, 368, 80)]
ORDERS = (RIGHT, LEFT)
NS = len(RIGHT)
LAST = NS - 1
DEPTH = 2
FIRST = (7, 5)
SIGN = (1, -1)


def wrapped(x):
    return x + N * (x < 0).astype(jnp.int32) - N * (x >= N).astype(jnp.int32)


def source(z, d, steps):
    return wrapped(z - SIGN[d] * steps)


def rows_of(d, k):
    return pl.ds(*ORDERS[d][k][1:])


def needs(d, k):
    hop, first, height = ORDERS[d][k]
    return [
        i for i, (h, f, n) in enumerate(ORDERS[d])
        if h == hop - 1 and f < first + height and first < f + n
    ]


def if_sent(z, d, k, act):
    if k < LAST:
        act()
    else:
        pl.when(z < N - 1 if d == 0 else z == 1)(act)


def if_received(z, d, k, act):
    if k < LAST:
        act()
    else:
        pl.when(z > 0 if d == 0 else z == 0)(act)


def exchange(
    wq, lq, hq, wk, lk, hk, wv, lv, hv, nt, ns,
    buf, gain,
    wq_v, wk_v, wv_v, lq_v, lk_v, lv_v, hq_v, hk_v, hv_v, nt_v, ns_v, gains,
    in_sem, send_sem, recv_sem, gsend, grecv, psend, precv, ready,
):
    count = [0]

    def load(src, dst):
        copy = pltpu.make_async_copy(src, dst, in_sem.at[count[0]])
        copy.start()
        count[0] += 1
        return copy

    got = {6: [load(lv, lv_v), load(hv, hv_v), load(wv, wv_v)]}
    got[0] = [load(lq, lq_v), load(hq, hq_v), load(wq.at[:, pl.ds(0, UNIT)], wq_v.at[0])]
    got_norm = [load(nt, nt_v), load(ns, ns_v)]
    got[5] = [load(lk, lk_v), load(hk, hk_v), load(wk, wk_v)]
    for i in (1, 4, 2, 3):
        got[i] = [load(wq.at[:, pl.ds(i * UNIT, UNIT)], wq_v.at[i])]

    z = lax.axis_index("rows")
    c = lax.axis_index("cols")
    to = (wrapped(z + 1), wrapped(z - 1))
    up, down = wrapped(c + 2), wrapped(c - 2)
    odd = lax.rem(c, 2)
    partner = c + 1 - 2 * odd
    barrier = pltpu.get_barrier_semaphore()

    def signal(sem, **who):
        pl.semaphore_signal(sem, inc=1, device_id=who, device_id_type=MESH)

    pl.when(z < N - 2)(lambda: signal(barrier, rows=to[0]))
    pl.when((z == 0) | (z == N - 1))(lambda: signal(barrier, rows=to[1]))
    pl.when(c < N - 2)(lambda: signal(barrier, cols=up))
    pl.when(c < 2)(lambda: signal(barrier, cols=down))
    pl.when(odd == 1)(lambda: signal(barrier, cols=partner))

    def greet(d):
        pl.when(z < N - 2 if d == 0 else rightmost)(lambda: pl.semaphore_wait(ready.at[d], 1))

    def compute(i):
        for x in got[i]:
            x.wait()
        w, h, lt = (
            (wq_v[i], hq_v[:, i * UNIT : (i + 1) * UNIT], lq_v[...]) if i < 5
            else (wk_v[...], hk_v[...], lk_v[...]) if i == 5
            else (wv_v[...], hv_v[...], lv_v[...])
        )
        delta = lax.dot_general(h, lt, (((0,), (0,)), ((), ())), preferred_element_type=F32)
        buf[z, pl.ds(i * UNIT, UNIT), :] = (w.T.astype(F32) + MIX * delta).astype(BF16)

    ahead = [(z > 0) & (z < N - 1), z >= N - 2, c >= 2, c >= N - 2, odd == 0]
    ahead = sum(x.astype(jnp.int32) for x in ahead)
    pl.when(ahead > 0)(lambda: pl.semaphore_wait(barrier, ahead))
    pl.when((z > 0) & (z < N - 1))(lambda: signal(ready.at[0], rows=to[1]))
    pl.when(z >= N - 2)(lambda: signal(ready.at[1], rows=to[0]))
    pl.when(c >= 2)(lambda: signal(ready.at[2], cols=down))
    pl.when(odd == 0)(lambda: signal(ready.at[3], cols=partner))

    rightmost = (z == 0) | (z == N - 1)

    @pl.when(rightmost)
    def _():
        compute(0)
        compute(6)

    @pl.when(jnp.logical_not(rightmost))
    def _():
        compute(6)
        compute(0)

    for x in got_norm:
        x.wait()
    gains[c, z, 0:1, 0:80] = (nt_v[...] + ns_v[...]).reshape(1, 80)

    def piece_copy(d, k, steps_more=0):
        ref = buf.at[source(z, d, ORDERS[d][k][0] + steps_more), rows_of(d, k), :]
        return pltpu.make_async_remote_copy(
            src_ref=ref, dst_ref=ref, send_sem=send_sem.at[d, k], recv_sem=recv_sem.at[d, k],
            device_id={"rows": to[d]}, device_id_type=MESH,
        )

    def gain_copy(d, hop, steps_more=0):
        ref = gains.at[c, source(z, d, hop + steps_more)]
        return pltpu.make_async_remote_copy(
            src_ref=ref, dst_ref=ref, send_sem=gsend.at[d, hop], recv_sem=grecv.at[d, hop],
            device_id={"rows": to[d]}, device_id_type=MESH,
        )

    def partner_copy(col):
        ref = gains.at[col]
        return pltpu.make_async_remote_copy(
            src_ref=ref, dst_ref=ref, send_sem=psend.at[0], recv_sem=precv.at[0],
            device_id={"cols": partner}, device_id_type=MESH,
        )

    def pair_copy(hop, steps_more=0):
        ref = gains.at[pl.ds(wrapped(c - odd - 2 * (hop + steps_more)), 2)]
        return pltpu.make_async_remote_copy(
            src_ref=ref, dst_ref=ref, send_sem=psend.at[1 + hop], recv_sem=precv.at[1 + hop],
            device_id={"cols": up}, device_id_type=MESH,
        )

    def norm_step(k):
        hop = {2: 1, 3: 2, 4: 3}.get(k)
        for d in range(2):
            if hop is not None and hop < 4 - d:
                gain_copy(d, hop - 1, 1).wait_recv()
                gain_copy(d, hop).start()

    def norm_end():
        gain_copy(1, 2, 1).wait_recv()
        gain_copy(0, 3, 1).wait_recv()
        pl.when(odd == 1)(lambda: pl.semaphore_wait(ready.at[3], 1))
        partner_copy(c).start()
        partner_copy(partner).wait_recv()
        pl.when(c < N - 2)(lambda: pl.semaphore_wait(ready.at[2], 1))
        for hop in range(3):
            pair_copy(hop).start()
            pair_copy(hop, 1).wait_recv()
        lane = lax.broadcasted_iota(jnp.int32, (N, PAD), 1)
        rows = [jnp.zeros((N, PAD), F32) for _ in range(5)]
        for j in range(N):
            row, off = divmod(80 * j, PAD)
            v = gains[j].reshape(N, PAD)
            v = pltpu.roll(v, off, 1) if off else v
            rows[row] = jnp.where((lane >= off) & (lane < off + 80), v, rows[row])
            if off + 80 > PAD:
                rows[row + 1] = jnp.where(lane < off + 80 - PAD, v, rows[row + 1])
        for j in range(5):
            gain[pl.ds(j, N, stride=5), :] = rows[j]
        for d in range(2):
            for hop in range(4 - d):
                gain_copy(d, hop).wait_send()
        partner_copy(c).wait_send()
        for hop in range(3):
            pair_copy(hop).wait_send()

    def begin(d):
        greet(d)
        gain_copy(d, 0).start()
        piece_copy(d, 0).start()

    def second(*ways):
        for d in ways:
            piece_copy(d, 1).start()

    @pl.when(z == 0)
    def _():
        begin(0)
        for i in (5, 1, 4, 2, 3):
            compute(i)
        second(0)
        begin(1)
        second(1)

    @pl.when(z == N - 1)
    def _():
        begin(0)
        compute(5)
        begin(1)
        for i in (1, 4, 2, 3):
            compute(i)
        second(0, 1)

    @pl.when(jnp.logical_not(rightmost))
    def _():
        begin(1)
        compute(5)
        begin(0)
        for i in (1, 4, 2, 3):
            compute(i)
        second(1, 0)

    def item(k, met):
        for d in (1, 0):
            for i in needs(d, k):
                if (d, i) not in met:
                    piece_copy(d, i, 1).wait_recv()
                    met.add((d, i))
            piece_copy(d, k - DEPTH).wait_send()
            piece_copy(d, k).start()

    def drain(last, met):
        for d in range(2):
            for k in range(last - DEPTH, last):
                piece_copy(d, k).wait_send()
            for k in range(last):
                if (d, k) not in met:
                    piece_copy(d, k, 1).wait_recv()

    met = set()
    low = min(FIRST)
    for k in range(DEPTH, low):
        norm_step(k)
        item(k, met)
    for parity in range(2):

        @pl.when(odd == parity)
        def _():
            mine = set(met)
            for k in range(low, FIRST[parity]):
                item(k, mine)
                if k == low:
                    norm_end()
            if FIRST[parity] == low:
                norm_end()
            drain(FIRST[parity], mine)


def finish(buf, late, send_sem, recv_sem):
    z = lax.axis_index("rows")
    odd = lax.rem(lax.axis_index("cols"), 2)
    to = (wrapped(z + 1), wrapped(z - 1))
    barrier = pltpu.get_barrier_semaphore()
    for d in range(2):
        pl.semaphore_signal(barrier, inc=1, device_id={"rows": to[d]}, device_id_type=MESH)
    pl.semaphore_wait(barrier, 2)

    low = min(FIRST)
    rest = max(FIRST)

    def piece_copy(d, k, first):
        hop = ORDERS[d][k][0]
        here = late.at[d] if needs(d, k)[0] >= first else buf.at[source(z, d, hop)]
        return pltpu.make_async_remote_copy(
            src_ref=here.at[rows_of(d, k), :], dst_ref=late.at[2 if hop == 3 else d, rows_of(d, k), :],
            send_sem=send_sem.at[0 if k < rest else 1 if k < LAST else 2 + d],
            recv_sem=recv_sem.at[2 * (k - low) + d if k < rest else 2 * (rest - low)],
            device_id={"rows": to[d]}, device_id_type=MESH,
        )

    def of_size(ref, send, recv):
        return pltpu.make_async_remote_copy(
            src_ref=ref, dst_ref=ref, send_sem=send_sem.at[send], recv_sem=recv_sem.at[recv],
            device_id={"rows": to[0]}, device_id_type=MESH,
        )

    for parity, first in enumerate(FIRST):

        @pl.when(odd == parity)
        def _():
            met = set()
            for k in range(first, NS):
                for d in (1, 0):
                    for i in needs(d, k):
                        if i >= first and (d, i) not in met:
                            piece_copy(d, i, first).wait_recv()
                            met.add((d, i))
                    if_sent(z, d, k, lambda d=d, k=k: piece_copy(d, k, first).start())
            for k in range(first, rest):
                for d in range(2):
                    if (d, k) not in met:
                        piece_copy(d, k, first).wait_recv()
            if first < rest:
                of_size(late.at[pl.ds(0, 2)], 0, 0).wait_send()
            sent = sum(ORDERS[d][rest][2] for d in range(2))
            of_size(late.at[2, pl.ds(0, sent), :], 1, 0).wait_send()
            for d in range(2):
                if_sent(z, d, LAST, lambda d=d: piece_copy(d, LAST, first).wait_send())
            of_size(late.at[2], 0, 2 * (rest - low)).wait_recv()


def write_out(outs, z, sem, blocks_of, blocks):
    for index, distance in blocks:
        block = blocks_of.at[index]
        at = pl.ds(pl.multiple_of(wrapped(z + distance) * ROWS, ROWS), ROWS)
        first = 0
        for out, width in zip(outs, COLS):
            pltpu.make_async_copy(block.at[pl.ds(first, width), :], out.at[:, at], sem.at[0]).start()
            first += width
    everything = blocks_of.at[pl.ds(0, len(blocks))]
    pltpu.make_async_copy(everything, everything, sem.at[0]).wait()


def early(parity):
    return (0, 1, -1, 2, -2) if FIRST[parity] == 5 else (0, 1, -1, 2, -2, 3, -3)


def deliver(buf, gain, q, k, v, g, sem):
    z = lax.axis_index("rows")
    odd = lax.rem(lax.axis_index("cols"), 2)
    g[...] = gain[...].astype(BF16)
    for parity in range(2):

        @pl.when(odd == parity)
        def _():
            write_out((q, k, v), z, sem, buf, [(wrapped(z + b), b) for b in early(parity)])


def deliver_late(late, q_in, k_in, v_in, q, k, v, sem):
    z = lax.axis_index("rows")
    odd = lax.rem(lax.axis_index("cols"), 2)
    for parity in range(2):

        @pl.when(odd == parity)
        def _():
            write_out((q, k, v), z, sem, late, [(slot, b) for slot, b in enumerate((-3, 3, 4)) if b not in early(parity)])


def local(wq, lq, hq, wk, lk, hk, wv, lv, hv, nt, ns):
    hbm = pl.BlockSpec(memory_space=pltpu.HBM)
    vmem = pl.BlockSpec(memory_space=pltpu.VMEM)
    dma = pltpu.SemaphoreType.DMA
    limit = 16 << 20
    args = (wq, lq.T, hq, wk, lk.T, hk, wv, lv.T, hv, nt, ns)
    buf, gain = pl.pallas_call(
        exchange,
        name="exchange",
        out_shape=(
            jax.ShapeDtypeStruct((N, WIDTH, ROWS), BF16),
            jax.ShapeDtypeStruct((40, PAD), F32),
        ),
        in_specs=[hbm] * 11,
        out_specs=(vmem, vmem),
        scratch_shapes=[
            pltpu.VMEM((5, ROWS, UNIT), BF16),
            pltpu.VMEM((ROWS, UNIT), BF16),
            pltpu.VMEM((ROWS, UNIT), BF16),
            pltpu.VMEM((32, ROWS), BF16),
            pltpu.VMEM((32, ROWS), BF16),
            pltpu.VMEM((32, ROWS), BF16),
            pltpu.VMEM((32, COLS[0]), BF16),
            pltpu.VMEM((32, COLS[1]), BF16),
            pltpu.VMEM((32, COLS[2]), BF16),
            pltpu.VMEM((80,), F32),
            pltpu.VMEM((80,), F32),
            pltpu.VMEM((N, N, 1, PAD), F32),
            dma((16,)),
            dma((2, NS)),
            dma((2, NS)),
            dma((2, 4)),
            dma((2, 4)),
            dma((4,)),
            dma((4,)),
            pltpu.SemaphoreType.REGULAR((4,)),
        ],
        compiler_params=pltpu.CompilerParams(collective_id=0, has_side_effects=True, vmem_limit_bytes=limit),
    )(*(pltpu.with_memory_space_constraint(x, pltpu.HBM) for x in args))
    wide = [jax.ShapeDtypeStruct((width, N * ROWS), BF16) for width in COLS]
    q, k, v, g = pl.pallas_call(
        deliver,
        name="deliver",
        out_shape=(*wide, jax.ShapeDtypeStruct((40, PAD), BF16)),
        in_specs=[vmem, vmem],
        out_specs=(hbm, hbm, hbm, vmem),
        scratch_shapes=[dma((1,))],
        compiler_params=pltpu.CompilerParams(vmem_limit_bytes=limit, has_side_effects=True),
    )(buf, gain)
    late = pl.pallas_call(
        finish,
        name="finish",
        out_shape=jax.ShapeDtypeStruct((3, WIDTH, ROWS), BF16),
        in_specs=[vmem],
        out_specs=vmem,
        scratch_shapes=[dma((4,)), dma((2 * (max(FIRST) - min(FIRST)) + 1,))],
        compiler_params=pltpu.CompilerParams(collective_id=1, has_side_effects=True, vmem_limit_bytes=limit),
    )(buf)
    q, k, v = pl.pallas_call(
        deliver_late,
        name="deliver_late",
        out_shape=tuple(wide),
        in_specs=[vmem, hbm, hbm, hbm],
        out_specs=(hbm, hbm, hbm),
        scratch_shapes=[dma((1,))],
        input_output_aliases={1: 0, 2: 1, 3: 2},
        compiler_params=pltpu.CompilerParams(vmem_limit_bytes=limit),
    )(late, q, k, v)
    return q, k, v, g.reshape(N * ROWS)


def solution(mesh):
    return jax.shard_map(
        local,
        mesh=mesh,
        in_specs=(
            P(("trial", "rows"), "cols"),
            P(("trial", "rows"), None),
            P("trial", "cols"),
            P(("trial", "rows"), "cols"),
            P(("trial", "rows"), None),
            P("trial", "cols"),
            P(("trial", "rows"), "cols"),
            P(("trial", "rows"), None),
            P("trial", "cols"),
            P(("trial", "rows", "cols")),
            P(("trial", "rows", "cols")),
        ),
        out_specs=(
            P(("trial", "cols"), None),
            P(("trial", "cols"), None),
            P(("trial", "cols"), None),
            P("trial"),
        ),
        check_vma=False,
    )
```
